128 devices in a mesh: grp: 32 (over x, z, y_lo), sub: 4 (over y_hi, core).
Axes of the slice: x: 4, y: 4 (y_hi: 2, y_lo: 2; y = y_hi * 2 + y_lo), z: 4, core: 2. Of those that a mesh axis runs over, the one named last changes fastest.
Arguments:
- gate_source: bfloat16 [128, 2048, 768], P('grp', 'sub'), may hold values from -0.125 to 0.125
- up_source: bfloat16 [128, 2048, 768], P('grp', 'sub'), may hold values from -0.125 to 0.125
- down_source: bfloat16 [128, 2048, 768], P('grp', 'sub'), may hold values from -0.21875 to 0.21875
- source_order: int32 [128], replicated, may hold values from 0 to 127, each once
- target_order: int32 [128], replicated, may hold values from 0 to 127, each once
Outputs:
- packed: bfloat16 [3, 32, 4, 8, 96, 2048], P(None, 'grp', 'sub')
- scales: float32 [3, 32, 4, 16, 768], P(None, 'grp', 'sub')
The draws below stay inside these ranges and needn't reach their ends.
Inputs may be any that keep to these rules, and one draw needn't show every extreme that they name: `source_order`: each expert number appears once. `target_order`: each expert number appears once.
All inputs are finite; a program needn't handle non-finite values. Where the reference program divides by a largest or mean magnitude, that divisor is 1e-20 or more.
Results may differ from the reference program's by a relative error of at most 0.001.
Values may be sent and summed in bfloat16 or wider, within the bound.
A program may use at most 192 MiB of HBM per device.

```python
import jax
import jax.numpy as jnp
from jax import lax

D = 2048
FF = 768
BLOCK = 128
E = 128
EPT = 8
FFT = 96
N_GRP = 32
N_SUB = 4


def levels(rng, shape, shards, smallest, largest):
    def one(position, blocks):
        steps = jax.random.uniform(jax.random.fold_in(jax.random.fold_in(rng, 6), position), (blocks,), jnp.float32, smallest / len(shards), largest / len(shards))
        return jnp.repeat(jnp.exp(steps), shape[position] // blocks).reshape((-1,) + (1,) * (len(shape) - position - 1))

    level = one(*shards[0])
    for cut in shards[1:]:
        level = level * one(*cut)
    return level


def bell_draw(own_key, shape, spread, most, cuts=(), kind=jnp.bfloat16):
    entries = spread * jax.random.normal(own_key, shape, jnp.float32)
    if cuts:
        entries = entries * levels(own_key, shape, cuts, -0.22, 0.18)
    return jnp.clip(entries, -most, most).astype(kind)


def setup_inputs(seed: int = 0) -> dict:
    splits = jax.random.split(jax.random.key(seed), 6)
    return {
        "gate_source": bell_draw(splits[0], (E, D, FF), D ** -0.5, 0.125, ((0, 32), (1, 4))),
        "up_source": bell_draw(splits[1], (E, D, FF), D ** -0.5, 0.125, ((0, 32), (1, 4))),
        "down_source": bell_draw(splits[2], (E, D, FF), FF ** -0.5, 0.21875, ((0, 32), (1, 4))),
        "source_order": jax.random.permutation(splits[3], E).astype(jnp.int32),
        "target_order": jax.random.permutation(splits[4], E).astype(jnp.int32),
    }


EPS = 1e-6


def pack_layout(quantized):
    values = quantized.reshape(N_GRP // 2, EPT, D, 2, N_SUB, FFT)
    values = values.transpose(0, 3, 4, 1, 5, 2)
    return values.reshape(N_GRP, N_SUB, EPT, FFT, D)


def scale_layout(block_scale):
    values = block_scale.reshape(N_GRP // 2, EPT, D // BLOCK, 2, N_SUB, FFT)
    values = values.transpose(0, 3, 4, 2, 1, 5)
    return values.reshape(N_GRP, N_SUB, D // BLOCK, EPT * FFT)


def convert(weights, picked):
    def convert_one(target):
        matrix = weights[picked[target]].astype(jnp.float32).reshape(D // BLOCK, BLOCK, FF)
        block_scale = jnp.max(jnp.abs(matrix), axis=1) + EPS
        quantized = (matrix / block_scale[:, None, :]).astype(jnp.bfloat16).reshape(D, FF)
        return quantized, block_scale

    quantized, block_scale = lax.map(convert_one, jnp.arange(E, dtype=jnp.int32))
    return pack_layout(quantized), scale_layout(block_scale)


def reference(gate_source, up_source, down_source, source_order, target_order):
    matches = (source_order[None, :] == target_order[:, None]).astype(jnp.int32)
    picked = jnp.sum(matches * jnp.arange(E, dtype=jnp.int32)[None, :], axis=1).astype(jnp.int32)
    gate_q, gate_s = convert(gate_source, picked)
    up_q, up_s = convert(up_source, picked)
    down_q, down_s = convert(down_source, picked)
    return jnp.stack([gate_q, up_q, down_q]), jnp.stack([gate_s, up_s, down_s])
```

```python
import functools

import jax
import jax.numpy as jnp
from jax import lax
from jax.experimental import pallas as pl
from jax.experimental.pallas import tpu as pltpu
from jax.sharding import PartitionSpec as P

BLOCK = 128
EPS = 1e-06
MESH = pl.DeviceIdType.MESH
MATS = 3
HOPS = (1, 3, 2)


def move_kernel(index_ref, gate, up, down, out, *scratch):
    first = scratch[0:3]
    second = scratch[3:6]
    own = scratch[6]
    turned = scratch[7:10]
    middle = scratch[10:13]
    sorted_ = scratch[13:16]
    relay = scratch[16:19]
    own_sem, first_send, first_recv, second_send, second_recv = scratch[19:24]
    y_send, y_recv, third_send, third_recv, last_send, last_recv, keep_sem = scratch[24:31]
    weights = (gate, up, down)

    g = lax.axis_index("grp")
    q = lax.axis_index("sub")
    x, z, yl = g // 8, (g // 2) % 4, g % 2
    core = q % 2
    s8 = yl * 4 + q

    def device(xx, zz, ss):
        return ((xx * 4 + zz) * 2 + ss // 4, ss % 4)

    def pick(a, b):
        return jnp.where(core == 0, a, b)

    def flip(a, b):
        low = (a + b) % 2
        high = (a // 2 + b // 2) % 2
        return high * 2 + low

    x_to = [(x + d) % 4 for d in range(4)]
    z_to = [(z + d) % 4 for d in range(4)]
    x_from = [(x + 4 - d) % 4 for d in range(4)]
    z_from = [(z + 4 - d) % 4 for d in range(4)]
    dev1 = [device(pick(x, x_to[d]), pick(z_to[d], z), s8) for d in range(4)]
    dev2 = [device(pick(x_to[d], x), pick(z, z_to[d]), s8) for d in range(4)]
    s8_to = [(flip((s8 // 4) * 2 + (s8 // 2) % 2, r // 2)) * 2 + (s8 + r) % 2 for r in range(8)]
    dev_y = [device(x, z, s8_to[r]) for r in range(8)]

    barrier = pltpu.get_barrier_semaphore()
    partners = dev1[1:] + dev2[1:] + dev_y[1:]
    for partner in partners:
        pl.semaphore_signal(barrier, inc=1, device_id=partner, device_id_type=MESH)
    pl.semaphore_wait(barrier, len(partners))

    tile2 = [pick(flip(q, x_to[d]), z_to[d]) for d in range(4)]

    def source(m, d1, t):
        slot = pick(t, flip(q, x_to[d1]))
        block = pick(z_to[d1], t)
        return weights[m].at[slot, pl.ds(pl.multiple_of(block * BLOCK, BLOCK), BLOCK), :]

    def first_copy(m, d1, d2):
        t = tile2[d2]
        return pltpu.make_async_remote_copy(
            src_ref=source(m, d1, t),
            dst_ref=first[m].at[d1 - 1, t],
            send_sem=first_send.at[m],
            recv_sem=first_recv.at[m, d1 - 1, t],
            device_id=dev1[d1],
            device_id_type=MESH,
        )

    def second_copy(m, d1, d2):
        t = tile2[d2]
        return pltpu.make_async_remote_copy(
            src_ref=source(m, 0, t) if d1 == 0 else first[m].at[d1 - 1, t],
            dst_ref=second[m].at[d2 - 1, d1],
            send_sem=second_send.at[m],
            recv_sem=second_recv.at[m, d2 - 1, d1],
            device_id=dev2[d2],
            device_id_type=MESH,
        )

    def own_copy(m):
        return pltpu.make_async_copy(source(m, 0, tile2[0]), own.at[m], own_sem.at[m])

    def start_first(m):
        for d2 in (1, 3, 2, 0):
            for d1 in HOPS:
                first_copy(m, d1, d2).start()
        for d2 in HOPS:
            second_copy(m, 0, d2).start()
        own_copy(m).start()

    def forward(m):
        for d2 in (1, 3, 2, 0):
            for d1 in HOPS:
                first_copy(m, d1, d2).wait_recv()
                if d2:
                    second_copy(m, d1, d2).start()

    units, columns = turned[0].shape[1], turned[0].shape[2]

    def y_copy(m, r):
        return pltpu.make_async_remote_copy(
            src_ref=turned[m].at[:, s8_to[r]],
            dst_ref=middle[m].at[pl.ds(s8 * 16, 16)],
            send_sem=y_send.at[m],
            recv_sem=y_recv.at[m, r - 1],
            device_id=dev_y[r],
            device_id_type=MESH,
        )

    def place_of(d1, d2):
        return pick(x_from[d2] * 4 + z_from[d1], x_from[d1] * 4 + z_from[d2])

    def turn_and_cross(m):
        own_copy(m).wait()

        def turn(tile, place):
            turned[m][place] = tile.T.reshape(units, columns, BLOCK)

        turn(own[m], place_of(0, 0))
        for d1 in HOPS:
            turn(first[m][d1 - 1, tile2[0]], place_of(d1, 0))
        for d1 in (0,) + HOPS:
            for d2 in HOPS:
                second_copy(m, d1, d2).wait_recv()
                turn(second[m][d2 - 1, d1], place_of(d1, d2))
        for r in range(1, 8):
            y_copy(m, r).start()
        middle[m][pl.ds(s8 * 16, 16)] = turned[m][:, s8]

    def third_copy(m, d1, t):
        return pltpu.make_async_remote_copy(
            src_ref=sorted_[m].at[pick(t, x_to[d1]), pick(z_to[d1], t)],
            dst_ref=relay[m].at[d1 - 1, t],
            send_sem=third_send.at[m],
            recv_sem=third_recv.at[m, d1 - 1, t],
            device_id=dev1[d1],
            device_id_type=MESH,
        )

    def last_source(m, d1, d2):
        t = pick(x_to[d2], z_to[d2])
        if d1 == 0:
            return sorted_[m].at[pick(t, x), pick(z, t)]
        return relay[m].at[d1 - 1, t]

    def last_place(m, d1):
        return out.at[m, pick(x * 4 + z_from[d1], x_from[d1] * 4 + z)]

    def last_copy(m, d1, d2):
        return pltpu.make_async_remote_copy(
            src_ref=last_source(m, d1, d2),
            dst_ref=last_place(m, d1),
            send_sem=last_send.at[m],
            recv_sem=last_recv.at[m],
            device_id=dev2[d2],
            device_id_type=MESH,
        )

    def keep_copy(m, d1):
        return pltpu.make_async_copy(last_source(m, d1, 0), last_place(m, d1), keep_sem.at[m, d1])

    def third_tile(d2):
        return pick(x_to[d2], z_to[d2])

    def permute(m):
        for r in range(1, 8):
            y_copy(m, r).wait_recv()

        def step(t, carry):
            for k in range(8):
                sorted_[m][t // 4, t % 4, k] = middle[m][index_ref[t * 8 + k]]
            return carry

        lax.fori_loop(0, 16, step, 0)
        for d2 in (1, 3, 2, 0):
            for d1 in HOPS:
                third_copy(m, d1, third_tile(d2)).start()
        for d2 in HOPS:
            last_copy(m, 0, d2).start()
        keep_copy(m, 0).start()

    def finish(m):
        for d2 in (1, 3, 2, 0):
            for d1 in HOPS:
                third_copy(m, d1, third_tile(d2)).wait_recv()
                if d2:
                    last_copy(m, d1, d2).start()
                else:
                    keep_copy(m, d1).start()

    start_first(0)
    start_first(1)
    start_first(2)
    forward(0)
    forward(1)
    turn_and_cross(0)
    forward(2)
    turn_and_cross(1)
    permute(0)
    turn_and_cross(2)
    finish(0)
    permute(1)
    finish(1)
    permute(2)
    finish(2)

    def drain(ref, sem):
        pltpu.make_async_copy(ref, ref, sem).wait()

    for m in range(MATS):
        drain(first[m], first_send.at[m])
        drain(second[m], second_send.at[m])
        drain(middle[m].at[pl.ds(0, 112)], y_send.at[m])
        drain(relay[m], third_send.at[m])
        drain(relay[m], last_send.at[m])
        drain(relay[m], last_recv.at[m])
        for d1 in range(4):
            keep_copy(m, d1).wait()


def scale_kernel(low_ref, moved, packed, scales):
    blocks = moved.shape[1]
    columns = moved.shape[3]
    k = pl.program_id(1)
    low = low_ref[k]
    found = []
    for b in range(blocks):
        place = ((b // 4) ^ low) * 4 + b % 4
        values = moved[0, place, 0].astype(jnp.float32)
        scale = jnp.max(jnp.abs(values), axis=1, keepdims=True) + EPS
        packed[0, 0, 0, 0, :, b * BLOCK : (b + 1) * BLOCK] = (values * (1.0 / scale)).astype(jnp.bfloat16)
        found.append(scale)
    scales[0, 0] = jnp.concatenate(found, axis=1).T


def per_device(gate, up, down, source_order, target_order):
    slots, rows, hidden = gate.shape
    columns = hidden // 8
    experts = source_order.shape[0]
    matches = (source_order[None, :] == target_order[:, None]).astype(jnp.int32)
    picked = jnp.sum(matches * jnp.arange(experts, dtype=jnp.int32)[None, :], axis=1)
    g = lax.axis_index("grp")
    x = g // 8
    col, yl, low = picked // 8, (picked // 4) % 2, picked % 4
    index = (yl * 4 + (low ^ x)) * 16 + col

    tile = (BLOCK, hidden)
    brick = (columns, BLOCK)
    bf16 = jnp.bfloat16
    dma = pltpu.SemaphoreType.DMA
    any_space = pl.BlockSpec(memory_space=pl.ANY)
    scratch = (
        [pltpu.VMEM((3, 4) + tile, bf16)] * 3
        + [pltpu.VMEM((3, 4) + tile, bf16)] * 3
        + [pltpu.VMEM((3,) + tile, bf16)]
        + [pltpu.VMEM((16, 8) + brick, bf16)] * 3
        + [pltpu.VMEM((128,) + brick, bf16)] * 3
        + [pltpu.VMEM((4, 4, 8) + brick, bf16)] * 3
        + [pltpu.VMEM((3, 4, 8) + brick, bf16)] * 3
        + [dma((3,)), dma((3,)), dma((3, 3, 4)), dma((3,)), dma((3, 3, 4))]
        + [dma((3,)), dma((3, 7)), dma((3,)), dma((3, 3, 4)), dma((3,)), dma((3,)), dma((3, 4))]
    )
    moved = pl.pallas_call(
        move_kernel,
        out_shape=jax.ShapeDtypeStruct((3, 16, 8) + brick, bf16),
        in_specs=[pl.BlockSpec(memory_space=pltpu.SMEM), any_space, any_space, any_space],
        out_specs=any_space,
        scratch_shapes=scratch,
        compiler_params=pltpu.CompilerParams(
            collective_id=0, has_side_effects=True, vmem_limit_bytes=60 * 2**20
        ),
        name="move",
    )(index, gate, up, down)

    mine = lax.dynamic_slice(low, ((g // 2) * 8,), (8,))
    packed, found = pl.pallas_call(
        scale_kernel,
        grid_spec=pltpu.PrefetchScalarGridSpec(
            num_scalar_prefetch=1,
            grid=(3, 8),
            in_specs=[pl.BlockSpec((1, 16, 1) + brick, lambda m, k, low: (m, 0, k, 0, 0))],
            out_specs=[
                pl.BlockSpec((1, 1, 1, 1, columns, 16 * BLOCK), lambda m, k, low: (m, 0, 0, k, 0, 0)),
                pl.BlockSpec((1, 1, 16, columns), lambda m, k, low: (m, k, 0, 0)),
            ],
        ),
        out_shape=[
            jax.ShapeDtypeStruct((3, 1, 1, 8, columns, 16 * BLOCK), bf16),
            jax.ShapeDtypeStruct((3, 8, 16, columns), jnp.float32),
        ],
        name="scale",
    )(mine, moved)
    scales = found.transpose(0, 2, 1, 3).reshape(3, 1, 1, 16, hidden)
    return packed, scales


def solution(mesh):
    placed = (P("grp", "sub", None), P("grp", "sub", None), P("grp", "sub", None), P(), P())
    return jax.shard_map(
        per_device,
        mesh=mesh,
        in_specs=placed,
        out_specs=(P(None, "grp", "sub", None, None, None), P(None, "grp", "sub", None, None)),
        check_vma=False,
    )
```

```python
import functools

import jax
import jax.numpy as jnp
from jax import lax
from jax.experimental import pallas as pl
from jax.experimental.pallas import tpu as pltpu
from jax.sharding import PartitionSpec as P

BLOCK = 128
EPS = 1e-06
MESH = pl.DeviceIdType.MESH
MATS = 3
HOPS = (1, 3, 2)


def move_kernel(index_ref, gate, up, down, out, *scratch):
    first = scratch[0:3]
    second = scratch[3:6]
    own = scratch[6]
    turned = scratch[7:10]
    middle = scratch[10:13]
    sorted_ = scratch[13:16]
    relay = scratch[16:19]
    own_sem, first_send, first_recv, second_send, second_recv = scratch[19:24]
    y_send, y_recv, third_send, third_recv, last_send, last_recv, keep_sem = scratch[24:31]
    weights = (gate, up, down)

    g = lax.axis_index("grp")
    q = lax.axis_index("sub")
    x, z, yl = g // 8, (g // 2) % 4, g % 2
    core = q % 2
    s8 = yl * 4 + q

    def device(xx, zz, ss):
        return ((xx * 4 + zz) * 2 + ss // 4, ss % 4)

    def pick(a, b):
        return jnp.where(core == 0, a, b)

    def flip(a, b):
        low = (a + b) % 2
        high = (a // 2 + b // 2) % 2
        return high * 2 + low

    x_to = [(x + d) % 4 for d in range(4)]
    z_to = [(z + d) % 4 for d in range(4)]
    x_from = [(x + 4 - d) % 4 for d in range(4)]
    z_from = [(z + 4 - d) % 4 for d in range(4)]
    dev1 = [device(pick(x, x_to[d]), pick(z_to[d], z), s8) for d in range(4)]
    dev2 = [device(pick(x_to[d], x), pick(z, z_to[d]), s8) for d in range(4)]
    s8_to = [(flip((s8 // 4) * 2 + (s8 // 2) % 2, r // 2)) * 2 + (s8 + r) % 2 for r in range(8)]
    dev_y = [device(x, z, s8_to[r]) for r in range(8)]

    barrier = pltpu.get_barrier_semaphore()
    partners = dev1[1:] + dev2[1:] + dev_y[1:]
    for partner in partners:
        pl.semaphore_signal(barrier, inc=1, device_id=partner, device_id_type=MESH)
    pl.semaphore_wait(barrier, len(partners))

    tile2 = [pick(flip(q, x_to[d]), z_to[d]) for d in range(4)]

    def source(m, d1, t):
        slot = pick(t, flip(q, x_to[d1]))
        block = pick(z_to[d1], t)
        return weights[m].at[slot, pl.ds(pl.multiple_of(block * BLOCK, BLOCK), BLOCK), :]

    def first_copy(m, d1, d2):
        t = tile2[d2]
        return pltpu.make_async_remote_copy(
            src_ref=source(m, d1, t),
            dst_ref=first[m].at[d1 - 1, t],
            send_sem=first_send.at[m],
            recv_sem=first_recv.at[m, d1 - 1, t],
            device_id=dev1[d1],
            device_id_type=MESH,
        )

    def second_copy(m, d1, d2):
        t = tile2[d2]
        return pltpu.make_async_remote_copy(
            src_ref=source(m, 0, t) if d1 == 0 else first[m].at[d1 - 1, t],
            dst_ref=second[m].at[d2 - 1, d1],
            send_sem=second_send.at[m],
            recv_sem=second_recv.at[m, d2 - 1, d1],
            device_id=dev2[d2],
            device_id_type=MESH,
        )

    def own_copy(m):
        return pltpu.make_async_copy(source(m, 0, tile2[0]), own.at[m], own_sem.at[m])

    def start_first(m):
        for d2 in (1, 3, 2, 0):
            for d1 in HOPS:
                first_copy(m, d1, d2).start()
        for d2 in HOPS:
            second_copy(m, 0, d2).start()
        own_copy(m).start()

    def forward(m):
        for d2 in (1, 3, 2, 0):
            for d1 in HOPS:
                first_copy(m, d1, d2).wait_recv()
                if d2:
                    second_copy(m, d1, d2).start()

    units, columns = turned[0].shape[1], turned[0].shape[2]

    def y_copy(m, r):
        return pltpu.make_async_remote_copy(
            src_ref=turned[m].at[:, s8_to[r]],
            dst_ref=middle[m].at[pl.ds(s8 * 16, 16)],
            send_sem=y_send.at[m],
            recv_sem=y_recv.at[m, r - 1],
            device_id=dev_y[r],
            device_id_type=MESH,
        )

    def place_of(d1, d2):
        return pick(x_from[d2] * 4 + z_from[d1], x_from[d1] * 4 + z_from[d2])

    def turn_and_cross(m):
        own_copy(m).wait()

        def turn(tile, place):
            turned[m][place] = tile.T.reshape(units, columns, BLOCK)

        turn(own[m], place_of(0, 0))
        for d1 in HOPS:
            turn(first[m][d1 - 1, tile2[0]], place_of(d1, 0))
        for d1 in (0,) + HOPS:
            for d2 in HOPS:
                second_copy(m, d1, d2).wait_recv()
                turn(second[m][d2 - 1, d1], place_of(d1, d2))
        for r in range(1, 8):
            y_copy(m, r).start()
        middle[m][pl.ds(s8 * 16, 16)] = turned[m][:, s8]

    def third_copy(m, d1, t):
        return pltpu.make_async_remote_copy(
            src_ref=sorted_[m].at[pick(t, x_to[d1]), pick(z_to[d1], t)],
            dst_ref=relay[m].at[d1 - 1, t],
            send_sem=third_send.at[m],
            recv_sem=third_recv.at[m, d1 - 1, t],
            device_id=dev1[d1],
            device_id_type=MESH,
        )

    def last_source(m, d1, d2):
        t = pick(x_to[d2], z_to[d2])
        if d1 == 0:
            return sorted_[m].at[pick(t, x), pick(z, t)]
        return relay[m].at[d1 - 1, t]

    def last_place(m, d1):
        return out.at[m, pick(x * 4 + z_from[d1], x_from[d1] * 4 + z)]

    def last_copy(m, d1, d2):
        return pltpu.make_async_remote_copy(
            src_ref=last_source(m, d1, d2),
            dst_ref=last_place(m, d1),
            send_sem=last_send.at[m],
            recv_sem=last_recv.at[m],
            device_id=dev2[d2],
            device_id_type=MESH,
        )

    def keep_copy(m, d1):
        return pltpu.make_async_copy(last_source(m, d1, 0), last_place(m, d1), keep_sem.at[m, d1])

    def third_tile(d2):
        return pick(x_to[d2], z_to[d2])

    def permute(m):
        for r in range(1, 8):
            y_copy(m, r).wait_recv()

        def step(t, carry):
            for k in range(8):
                sorted_[m][t // 4, t % 4, k] = middle[m][index_ref[t * 8 + k]]
            return carry

        lax.fori_loop(0, 16, step, 0)
        for d2 in (1, 3, 2, 0):
            for d1 in HOPS:
                third_copy(m, d1, third_tile(d2)).start()
        for d2 in HOPS:
            last_copy(m, 0, d2).start()
        keep_copy(m, 0).start()

    def finish(m):
        for d2 in (1, 3, 2, 0):
            for d1 in HOPS:
                third_copy(m, d1, third_tile(d2)).wait_recv()
                if d2:
                    last_copy(m, d1, d2).start()
                else:
                    keep_copy(m, d1).start()

    start_first(0)
    start_first(1)
    start_first(2)
    forward(0)
    forward(1)
    turn_and_cross(0)
    forward(2)
    turn_and_cross(1)
    permute(0)
    turn_and_cross(2)
    finish(0)
    permute(1)
    finish(1)
    permute(2)
    finish(2)

    def drain(ref, sem):
        pltpu.make_async_copy(ref, ref, sem).wait()

    for m in range(MATS):
        drain(first[m], first_send.at[m])
        drain(second[m], second_send.at[m])
        drain(middle[m].at[pl.ds(0, 112)], y_send.at[m])
        drain(relay[m], third_send.at[m])
        drain(relay[m], last_send.at[m])
        drain(relay[m], last_recv.at[m])
        for d1 in range(4):
            keep_copy(m, d1).wait()


def scale_kernel(low_ref, moved, packed, scales, ready, found, sem):
    columns = moved.shape[3]
    lane = lax.broadcasted_iota(jnp.int32, (columns, BLOCK), 1)

    def out_copy(m, k):
        return pltpu.make_async_copy(ready.at[m, k], packed.at[m, 0, 0, k], sem.at[m, k])

    for m in range(MATS):

        def step(k, carry):
            low = low_ref[k]
            seen = jnp.zeros((columns, BLOCK), jnp.float32)
            for b in range(16):
                place = ((b // 4) ^ low) * 4 + b % 4
                values = moved[m, place, k].astype(jnp.float32)
                scale = jnp.max(jnp.abs(values), axis=1, keepdims=True) + EPS
                ready[m, k, :, b * BLOCK : (b + 1) * BLOCK] = (values * (1.0 / scale)).astype(jnp.bfloat16)
                seen = jnp.where(lane == b, scale, seen)
            found[k] = seen.T[:16]
            out_copy(m, k).start()
            return carry

        lax.fori_loop(0, 8, step, 0)
        scales[m, 0, 0] = jnp.concatenate([found[k] for k in range(8)], axis=1)

    for m in range(MATS):
        for k in range(8):
            out_copy(m, k).wait()


def per_device(gate, up, down, source_order, target_order):
    slots, rows, hidden = gate.shape
    columns = hidden // 8
    experts = source_order.shape[0]
    matches = (source_order[None, :] == target_order[:, None]).astype(jnp.int32)
    picked = jnp.sum(matches * jnp.arange(experts, dtype=jnp.int32)[None, :], axis=1)
    g = lax.axis_index("grp")
    x = g // 8
    col, yl, low = picked // 8, (picked // 4) % 2, picked % 4
    index = (yl * 4 + (low ^ x)) * 16 + col

    tile = (BLOCK, hidden)
    brick = (columns, BLOCK)
    bf16 = jnp.bfloat16
    dma = pltpu.SemaphoreType.DMA
    any_space = pl.BlockSpec(memory_space=pl.ANY)
    scratch = (
        [pltpu.VMEM((3, 4) + tile, bf16)] * 3
        + [pltpu.VMEM((3, 4) + tile, bf16)] * 3
        + [pltpu.VMEM((3,) + tile, bf16)]
        + [pltpu.VMEM((16, 8) + brick, bf16)] * 3
        + [pltpu.VMEM((128,) + brick, bf16)] * 3
        + [pltpu.VMEM((4, 4, 8) + brick, bf16)] * 3
        + [pltpu.VMEM((3, 4, 8) + brick, bf16)] * 3
        + [dma((3,)), dma((3,)), dma((3, 3, 4)), dma((3,)), dma((3, 3, 4))]
        + [dma((3,)), dma((3, 7)), dma((3,)), dma((3, 3, 4)), dma((3,)), dma((3,)), dma((3, 4))]
    )
    moved = pl.pallas_call(
        move_kernel,
        out_shape=pltpu.VMEM((3, 16, 8) + brick, bf16),
        in_specs=[pl.BlockSpec(memory_space=pltpu.SMEM), any_space, any_space, any_space],
        out_specs=pl.BlockSpec(memory_space=pltpu.VMEM),
        scratch_shapes=scratch,
        compiler_params=pltpu.CompilerParams(
            collective_id=0, has_side_effects=True, vmem_limit_bytes=51 * 2**20
        ),
        name="move",
    )(index, gate, up, down)

    mine = lax.dynamic_slice(low, ((g // 2) * 8,), (8,))
    return pl.pallas_call(
        scale_kernel,
        in_specs=[pl.BlockSpec(memory_space=pltpu.SMEM), pl.BlockSpec(memory_space=pltpu.VMEM)],
        out_specs=[any_space, pl.BlockSpec(memory_space=pltpu.VMEM)],
        out_shape=[
            jax.ShapeDtypeStruct((3, 1, 1, 8, columns, 16 * BLOCK), bf16),
            jax.ShapeDtypeStruct((3, 1, 1, 16, hidden), jnp.float32),
        ],
        scratch_shapes=[pltpu.VMEM((3, 8, columns, 16 * BLOCK), bf16), pltpu.VMEM((8, 16, columns), jnp.float32), dma((3, 8))],
        compiler_params=pltpu.CompilerParams(vmem_limit_bytes=20 * 2**20),
        name="scale",
    )(mine, moved)


def solution(mesh):
    placed = (P("grp", "sub", None), P("grp", "sub", None), P("grp", "sub", None), P(), P())
    return jax.shard_map(
        per_device,
        mesh=mesh,
        in_specs=placed,
        out_specs=(P(None, "grp", "sub", None, None, None), P(None, "grp", "sub", None, None)),
        check_vma=False,
    )
```

```python
import functools

import jax
import jax.numpy as jnp
from jax import lax
from jax.experimental import pallas as pl
from jax.experimental.pallas import tpu as pltpu
from jax.sharding import PartitionSpec as P

BLOCK = 128
EPS = 1e-06
MESH = pl.DeviceIdType.MESH
MATS = 3
HOPS = (1, 3, 2)
ROOMS = ((12, 11), (13, 12), (14, 14))


def device(x, z, s8):
    return ((x * 4 + z) * 2 + s8 // 4, s8 % 4)


def flip(a, b):
    low = (a + b) % 2
    high = (a // 2 + b // 2) % 2
    return high * 2 + low


def place():
    g = lax.axis_index("grp")
    q = lax.axis_index("sub")
    return g // 8, (g // 2) % 4, g % 2, q


def greet(partners):
    barrier = pltpu.get_barrier_semaphore()
    for partner in partners:
        pl.semaphore_signal(barrier, inc=1, device_id=partner, device_id_type=MESH)
    pl.semaphore_wait(barrier, len(partners))


def drain(ref, sem):
    pltpu.make_async_copy(ref, ref, sem).wait()


def crossings(s8):
    return [flip((s8 // 4) * 2 + (s8 // 2) % 2, r // 2) * 2 + (s8 + r) % 2 for r in range(8)]


def plan_kernel(source_ref, target_ref, table_ref, level_ref):
    x, z, _, _ = place()
    f32, i32 = jnp.float32, jnp.int32
    shape = (128, 128)
    row = lax.broadcasted_iota(i32, shape, 0)
    lane = lax.broadcasted_iota(i32, shape, 1)
    source = jnp.broadcast_to(source_ref[...].astype(f32), shape).T
    target = jnp.broadcast_to(target_ref[...].astype(f32), shape)
    found = jnp.where(source == target, lane.astype(f32), 0.0)
    to = jnp.broadcast_to(jnp.sum(found, axis=1, keepdims=True), shape).astype(i32)
    x_to, z_to = to // 32, (to // 8) % 4
    x_at, z_at = row // 32, (row // 8) % 4
    inner = ((row // 4) % 2) * 32 + row % 4

    def down(values):
        return jnp.sum(values.astype(f32), axis=0, keepdims=True).astype(i32)

    worst = [jnp.zeros(shape, f32)] * 2
    for kind in range(2):
        at, end, mine = (x_at, x_to, x) if kind == 0 else (z_at, z_to, z)
        key = (at * 4 + end).astype(f32)
        same = jnp.where((key == key.T) & (lane < row), 1.0, 0.0)
        rank = jnp.broadcast_to(jnp.sum(same, axis=1, keepdims=True), shape).astype(i32)
        away = (end - at + 4) % 4
        index = kind * 64 + inner + (z_at if kind == 0 else x_at) * 4
        sent = (at == mine) & (away == lane // 32 + 1) & (rank == lane % 32)
        step = lane // 8
        if kind == 0:
            slot = (x * 4 + (z + step) % 4) * 8 + lane % 8
        else:
            slot = (((x + step) % 4) * 4 + z) * 8 + lane % 8
        got = (to == slot) & (lane < 32)
        base = kind * 5
        table_ref[base : base + 1, :] = down(jnp.where(sent, index, 0))
        table_ref[base + 1 : base + 2, :] = down(jnp.where(got & (away == 0), index, 0))
        table_ref[base + 2 : base + 3, :] = down(jnp.where(got & (away > 0), away - 1, 0))
        table_ref[base + 3 : base + 4, :] = down(jnp.where(got & (away > 0), rank, 0))
        table_ref[base + 4 : base + 5, :] = down(jnp.where(got & (away == 0), 1, 0))
        needed = (rank + 1).astype(f32)
        worst[0] = jnp.maximum(worst[0], jnp.where(away % 2 == 1, needed, 0.0))
        worst[1] = jnp.maximum(worst[1], jnp.where(away == 2, needed, 0.0))
    table_ref[10:16, :] = jnp.zeros((6, 128), i32)
    side, across = (jnp.max(values) for values in worst)
    level = jnp.int32(0)
    for near, far in ROOMS:
        level += ((side > near) | (across > far)).astype(i32)
    level_ref[0] = level


def quantize(load, store, columns):
    lane = lax.broadcasted_iota(jnp.int32, (columns, BLOCK), 1)
    seen = jnp.zeros((columns, BLOCK), jnp.float32)
    for b in range(16):
        values = load(b).astype(jnp.float32)
        scale = jnp.max(jnp.abs(values), axis=1, keepdims=True) + EPS
        store(b, (values * (1.0 / scale)).astype(jnp.bfloat16))
        seen = jnp.where(lane == b, scale, seen)
    return seen.T[:16]


def direct_kernel(room, table, gate, up, down, out, scales, *scratch):
    first = scratch[0:3]
    own = scratch[3]
    turned = scratch[4:7]
    middle = scratch[7:10]
    packs = scratch[10:12]
    landed = scratch[12:15]
    found = scratch[15]
    own_sem, first_send, first_recv, y_send, y_recv = scratch[16:21]
    direct_send, direct_recv, last_send, last_recv = scratch[21:25]
    weights = (gate, up, down)
    slots = (0, room[0], room[1], room[0])

    def drain_direct(m):
        for kind in range(2):
            for d in HOPS:
                drain(packs[0].at[kind, d - 1, pl.ds(0, slots[d])], direct_send.at[m, kind, d - 1])

    x, z, yl, q = place()
    core = q % 2
    s8 = yl * 4 + q
    units, columns = turned[0].shape[1], turned[0].shape[2]

    def pick(a, b):
        return jnp.where(core == 0, a, b)

    x_to = [device((x + d) % 4, z, s8) for d in range(4)]
    z_to = [device(x, (z + d) % 4, s8) for d in range(4)]
    s8_to = crossings(s8)
    y_to = [device(x, z, s) for s in s8_to]
    greet(x_to[1:] + z_to[1:] + y_to[1:])

    spot = pick(z, x)

    def rows(m, d):
        block = (spot + d) % 4
        return weights[m].at[:, pl.ds(pl.multiple_of(block * BLOCK, BLOCK), BLOCK), :]

    def first_copy(m, d):
        return pltpu.make_async_remote_copy(
            src_ref=rows(m, d),
            dst_ref=first[m].at[d - 1],
            send_sem=first_send.at[m],
            recv_sem=first_recv.at[m, d - 1],
            device_id=tuple(pick(a, b) for a, b in zip(z_to[d], x_to[d])),
            device_id_type=MESH,
        )

    def own_copy(m):
        return pltpu.make_async_copy(rows(m, 0), own.at[m], own_sem.at[m])

    slot = (core * 4 + yl * 2 + q // 2) * 16

    def origin(d):
        return ((spot + 4 - d) % 4) * 4

    def y_copy(m, d, r):
        return pltpu.make_async_remote_copy(
            src_ref=turned[m].at[pl.ds(origin(d), 4), s8_to[r]],
            dst_ref=middle[m].at[pl.ds(slot + origin(d), 4)],
            send_sem=y_send.at[m],
            recv_sem=y_recv.at[m, r - 1],
            device_id=y_to[r],
            device_id_type=MESH,
        )

    def direct_copy(m, kind, d):
        return pltpu.make_async_remote_copy(
            src_ref=packs[m % 2].at[kind, d - 1, pl.ds(0, slots[d])],
            dst_ref=landed[m].at[kind, d - 1, pl.ds(0, slots[d])],
            send_sem=direct_send.at[m, kind, d - 1],
            recv_sem=direct_recv.at[m, kind, d - 1],
            device_id=(x_to, z_to)[kind][d],
            device_id_type=MESH,
        )

    def last_copy(m, kind, d):
        return pltpu.make_async_remote_copy(
            src_ref=turned[m].at[pl.ds((kind * 3 + d - 1) * 2, 2)],
            dst_ref=out.at[m, kind, (z, x)[kind]],
            send_sem=last_send.at[m],
            recv_sem=last_recv.at[m, kind, d - 1],
            device_id=(z_to, x_to)[kind][d],
            device_id_type=MESH,
        )

    def start(m):
        for d in HOPS:
            first_copy(m, d).start()
        own_copy(m).start()

    def turn(m, d):
        if d:
            first_copy(m, d).wait_recv()
            tiles = first[m].at[d - 1]
        else:
            own_copy(m).wait()
            tiles = own.at[m]

        def one(i, carry):
            turned[m][origin(d) + i] = tiles[i].T.reshape(units, columns, BLOCK)
            return carry

        lax.fori_loop(0, 4, one, 0)
        for r in (2, 4, 6, 3, 5, 7, 1):
            y_copy(m, d, r).start()
        middle[m][pl.ds(slot + origin(d), 4)] = turned[m][pl.ds(origin(d), 4), s8]

    def gather(m):
        for r in range(1, 8):
            drain(middle[m].at[pl.ds(0, 16)], y_recv.at[m, r - 1])
        if m == 2:
            drain_direct(0)
        for d in HOPS:
            for kind in range(2):

                def one(r, carry):
                    index = table[kind * 5, (d - 1) * 32 + r]
                    for half in range(2):
                        packs[m % 2][kind, d - 1, r, half] = middle[m][index + 16 * half]
                    return carry

                lax.fori_loop(0, slots[d], one, 0)
                direct_copy(m, kind, d).start()

    def spread(m):
        for kind in range(2):
            for d in HOPS:
                direct_copy(m, kind, d).wait_recv()
        drain(turned[m].at[pl.ds(0, 14)], y_send.at[m])
        for d in HOPS + (0,):
            for kind in range(2):

                def one(k, carry):
                    spot_in = d * 8 + k
                    near = table[kind * 5 + 1, spot_in]
                    hop = table[kind * 5 + 2, spot_in]
                    rank = table[kind * 5 + 3, spot_in]
                    stay = table[kind * 5 + 4, spot_in] > 0
                    for half in range(2):
                        here = middle[m][near + 16 * half]
                        there = landed[m][kind, hop, rank, half]
                        brick = lax.select(jnp.broadcast_to(stay, here.shape), here, there)
                        if d == 0:
                            out[m, kind, (z, x)[kind], half, k] = brick
                        else:
                            turned[m][(kind * 3 + d - 1) * 2 + half, k] = brick
                    return carry

                lax.fori_loop(0, 8, one, 0)
                if d:
                    last_copy(m, kind, d).start()

    def settle(m):
        for kind in range(2):
            for d in HOPS:
                last_copy(m, kind, d).wait_recv()
        if m == MATS - 1:
            return

        def one(k, carry):
            def load(b):
                return out[m, (b // 4) % 2, b % 4, b // 8, k]

            def store(b, brick):
                out[m, (b // 4) % 2, b % 4, b // 8, k] = brick

            found[k] = quantize(load, store, columns)
            return carry

        lax.fori_loop(0, 8, one, 0)
        scales[m] = jnp.concatenate([found[k] for k in range(8)], axis=1)

    for m in range(MATS):
        start(m)
    turn(0, 0)
    turn(1, 0)
    for d in HOPS:
        turn(0, d)
    for d in HOPS:
        turn(1, d)
    turn(2, 0)
    gather(0)
    for d in HOPS:
        turn(2, d)
    gather(1)
    spread(0)
    gather(2)
    spread(1)
    settle(0)
    spread(2)
    settle(1)
    settle(2)

    for m in range(MATS):
        drain(first[m], first_send.at[m])
        if m:
            drain_direct(m)
        drain(turned[m].at[pl.ds(0, 12)], last_send.at[m])


def write_kernel(moved, early, packed, scales, ready, found, early_sem, sem):
    columns = moved.shape[-2]
    last = MATS - 1

    def early_copy(m, k, b):
        return pltpu.make_async_copy(
            moved.at[m, (b // 4) % 2, b % 4, b // 8, k],
            packed.at[m, 0, 0, k, :, pl.ds(b * BLOCK, BLOCK)],
            early_sem.at[m],
        )

    def late_copy(k):
        return pltpu.make_async_copy(ready.at[k], packed.at[last, 0, 0, k], sem.at[k])

    for m in range(last):

        def issue(k, carry):
            for b in range(16):
                early_copy(m, k, b).start()
            return carry

        lax.fori_loop(0, 8, issue, 0)

    def one(k, carry):
        def load(b):
            return moved[last, (b // 4) % 2, b % 4, b // 8, k]

        def store(b, brick):
            ready[k, :, b * BLOCK : (b + 1) * BLOCK] = brick

        found[k] = quantize(load, store, columns)
        late_copy(k).start()
        return carry

    lax.fori_loop(0, 8, one, 0)
    for m in range(last):
        scales[m, 0, 0] = early[m]
    scales[last, 0, 0] = jnp.concatenate([found[k] for k in range(8)], axis=1)
    for m in range(last):
        drain(packed.at[m], early_sem.at[m])
    for k in range(8):
        late_copy(k).wait()


def move_kernel(index_ref, gate, up, down, out, *scratch):
    first = scratch[0:3]
    second = scratch[3:6]
    own = scratch[6]
    turned = scratch[7:10]
    middle = scratch[10:13]
    sorted_ = scratch[13:16]
    relay = scratch[16:19]
    own_sem, first_send, first_recv, second_send, second_recv = scratch[19:24]
    y_send, y_recv, third_send, third_recv, last_send, last_recv, keep_sem = scratch[24:31]
    weights = (gate, up, down)

    g = lax.axis_index("grp")
    q = lax.axis_index("sub")
    x, z, yl = g // 8, (g // 2) % 4, g % 2
    core = q % 2
    s8 = yl * 4 + q

    def device(xx, zz, ss):
        return ((xx * 4 + zz) * 2 + ss // 4, ss % 4)

    def pick(a, b):
        return jnp.where(core == 0, a, b)

    def flip(a, b):
        low = (a + b) % 2
        high = (a // 2 + b // 2) % 2
        return high * 2 + low

    x_to = [(x + d) % 4 for d in range(4)]
    z_to = [(z + d) % 4 for d in range(4)]
    x_from = [(x + 4 - d) % 4 for d in range(4)]
    z_from = [(z + 4 - d) % 4 for d in range(4)]
    dev1 = [device(pick(x, x_to[d]), pick(z_to[d], z), s8) for d in range(4)]
    dev2 = [device(pick(x_to[d], x), pick(z, z_to[d]), s8) for d in range(4)]
    s8_to = [(flip((s8 // 4) * 2 + (s8 // 2) % 2, r // 2)) * 2 + (s8 + r) % 2 for r in range(8)]
    dev_y = [device(x, z, s8_to[r]) for r in range(8)]

    barrier = pltpu.get_barrier_semaphore()
    partners = dev1[1:] + dev2[1:] + dev_y[1:]
    for partner in partners:
        pl.semaphore_signal(barrier, inc=1, device_id=partner, device_id_type=MESH)
    pl.semaphore_wait(barrier, len(partners))

    tile2 = [pick(flip(q, x_to[d]), z_to[d]) for d in range(4)]

    def source(m, d1, t):
        slot = pick(t, flip(q, x_to[d1]))
        block = pick(z_to[d1], t)
        return weights[m].at[slot, pl.ds(pl.multiple_of(block * BLOCK, BLOCK), BLOCK), :]

    def first_copy(m, d1, d2):
        t = tile2[d2]
        return pltpu.make_async_remote_copy(
            src_ref=source(m, d1, t),
            dst_ref=first[m].at[d1 - 1, t],
            send_sem=first_send.at[m],
            recv_sem=first_recv.at[m, d1 - 1, t],
            device_id=dev1[d1],
            device_id_type=MESH,
        )

    def second_copy(m, d1, d2):
        t = tile2[d2]
        return pltpu.make_async_remote_copy(
            src_ref=source(m, 0, t) if d1 == 0 else first[m].at[d1 - 1, t],
            dst_ref=second[m].at[d2 - 1, d1],
            send_sem=second_send.at[m],
            recv_sem=second_recv.at[m, d2 - 1, d1],
            device_id=dev2[d2],
            device_id_type=MESH,
        )

    def own_copy(m):
        return pltpu.make_async_copy(source(m, 0, tile2[0]), own.at[m], own_sem.at[m])

    def start_first(m):
        for d2 in (1, 3, 2, 0):
            for d1 in HOPS:
                first_copy(m, d1, d2).start()
        for d2 in HOPS:
            second_copy(m, 0, d2).start()
        own_copy(m).start()

    def forward(m):
        for d2 in (1, 3, 2, 0):
            for d1 in HOPS:
                first_copy(m, d1, d2).wait_recv()
                if d2:
                    second_copy(m, d1, d2).start()

    units, columns = turned[0].shape[1], turned[0].shape[2]

    def y_copy(m, r):
        return pltpu.make_async_remote_copy(
            src_ref=turned[m].at[:, s8_to[r]],
            dst_ref=middle[m].at[pl.ds(s8 * 16, 16)],
            send_sem=y_send.at[m],
            recv_sem=y_recv.at[m, r - 1],
            device_id=dev_y[r],
            device_id_type=MESH,
        )

    def place_of(d1, d2):
        return pick(x_from[d2] * 4 + z_from[d1], x_from[d1] * 4 + z_from[d2])

    def turn_and_cross(m):
        own_copy(m).wait()

        def turn(tile, place):
            turned[m][place] = tile.T.reshape(units, columns, BLOCK)

        turn(own[m], place_of(0, 0))
        for d1 in HOPS:
            turn(first[m][d1 - 1, tile2[0]], place_of(d1, 0))
        for d1 in (0,) + HOPS:
            for d2 in HOPS:
                second_copy(m, d1, d2).wait_recv()
                turn(second[m][d2 - 1, d1], place_of(d1, d2))
        for r in range(1, 8):
            y_copy(m, r).start()
        middle[m][pl.ds(s8 * 16, 16)] = turned[m][:, s8]

    def third_copy(m, d1, t):
        return pltpu.make_async_remote_copy(
            src_ref=sorted_[m].at[pick(t, x_to[d1]), pick(z_to[d1], t)],
            dst_ref=relay[m].at[d1 - 1, t],
            send_sem=third_send.at[m],
            recv_sem=third_recv.at[m, d1 - 1, t],
            device_id=dev1[d1],
            device_id_type=MESH,
        )

    def last_source(m, d1, d2):
        t = pick(x_to[d2], z_to[d2])
        if d1 == 0:
            return sorted_[m].at[pick(t, x), pick(z, t)]
        return relay[m].at[d1 - 1, t]

    def last_place(m, d1):
        return out.at[m, pick(x * 4 + z_from[d1], x_from[d1] * 4 + z)]

    def last_copy(m, d1, d2):
        return pltpu.make_async_remote_copy(
            src_ref=last_source(m, d1, d2),
            dst_ref=last_place(m, d1),
            send_sem=last_send.at[m],
            recv_sem=last_recv.at[m],
            device_id=dev2[d2],
            device_id_type=MESH,
        )

    def keep_copy(m, d1):
        return pltpu.make_async_copy(last_source(m, d1, 0), last_place(m, d1), keep_sem.at[m, d1])

    def third_tile(d2):
        return pick(x_to[d2], z_to[d2])

    def permute(m):
        for r in range(1, 8):
            y_copy(m, r).wait_recv()

        def step(t, carry):
            for k in range(8):
                sorted_[m][t // 4, t % 4, k] = middle[m][index_ref[t * 8 + k]]
            return carry

        lax.fori_loop(0, 16, step, 0)
        for d2 in (1, 3, 2, 0):
            for d1 in HOPS:
                third_copy(m, d1, third_tile(d2)).start()
        for d2 in HOPS:
            last_copy(m, 0, d2).start()
        keep_copy(m, 0).start()

    def finish(m):
        for d2 in (1, 3, 2, 0):
            for d1 in HOPS:
                third_copy(m, d1, third_tile(d2)).wait_recv()
                if d2:
                    last_copy(m, d1, d2).start()
                else:
                    keep_copy(m, d1).start()

    start_first(0)
    start_first(1)
    start_first(2)
    forward(0)
    forward(1)
    turn_and_cross(0)
    forward(2)
    turn_and_cross(1)
    permute(0)
    turn_and_cross(2)
    finish(0)
    permute(1)
    finish(1)
    permute(2)
    finish(2)

    def drain(ref, sem):
        pltpu.make_async_copy(ref, ref, sem).wait()

    for m in range(MATS):
        drain(first[m], first_send.at[m])
        drain(second[m], second_send.at[m])
        drain(middle[m].at[pl.ds(0, 112)], y_send.at[m])
        drain(relay[m], third_send.at[m])
        drain(relay[m], last_send.at[m])
        drain(relay[m], last_recv.at[m])
        for d1 in range(4):
            keep_copy(m, d1).wait()


def scale_kernel(low_ref, moved, packed, scales, ready, found, sem):
    columns = moved.shape[3]
    lane = lax.broadcasted_iota(jnp.int32, (columns, BLOCK), 1)

    def out_copy(m, k):
        return pltpu.make_async_copy(ready.at[m, k], packed.at[m, 0, 0, k], sem.at[m, k])

    for m in range(MATS):

        def step(k, carry):
            low = low_ref[k]
            seen = jnp.zeros((columns, BLOCK), jnp.float32)
            for b in range(16):
                place = ((b // 4) ^ low) * 4 + b % 4
                values = moved[m, place, k].astype(jnp.float32)
                scale = jnp.max(jnp.abs(values), axis=1, keepdims=True) + EPS
                ready[m, k, :, b * BLOCK : (b + 1) * BLOCK] = (values * (1.0 / scale)).astype(jnp.bfloat16)
                seen = jnp.where(lane == b, scale, seen)
            found[k] = seen.T[:16]
            out_copy(m, k).start()
            return carry

        lax.fori_loop(0, 8, step, 0)
        scales[m, 0, 0] = jnp.concatenate([found[k] for k in range(8)], axis=1)

    for m in range(MATS):
        for k in range(8):
            out_copy(m, k).wait()


def through(table, gate, up, down, source_order, target_order):
    slots, rows, hidden = gate.shape
    columns = hidden // 8
    experts = source_order.shape[0]
    matches = (source_order[None, :] == target_order[:, None]).astype(jnp.int32)
    picked = jnp.sum(matches * jnp.arange(experts, dtype=jnp.int32)[None, :], axis=1)
    g = lax.axis_index("grp")
    x = g // 8
    col, yl, low = picked // 8, (picked // 4) % 2, picked % 4
    index = (yl * 4 + (low ^ x)) * 16 + col

    tile = (BLOCK, hidden)
    brick = (columns, BLOCK)
    bf16 = jnp.bfloat16
    dma = pltpu.SemaphoreType.DMA
    any_space = pl.BlockSpec(memory_space=pl.ANY)
    scratch = (
        [pltpu.VMEM((3, 4) + tile, bf16)] * 3
        + [pltpu.VMEM((3, 4) + tile, bf16)] * 3
        + [pltpu.VMEM((3,) + tile, bf16)]
        + [pltpu.VMEM((16, 8) + brick, bf16)] * 3
        + [pltpu.VMEM((128,) + brick, bf16)] * 3
        + [pltpu.VMEM((4, 4, 8) + brick, bf16)] * 3
        + [pltpu.VMEM((3, 4, 8) + brick, bf16)] * 3
        + [dma((3,)), dma((3,)), dma((3, 3, 4)), dma((3,)), dma((3, 3, 4))]
        + [dma((3,)), dma((3, 7)), dma((3,)), dma((3, 3, 4)), dma((3,)), dma((3,)), dma((3, 4))]
    )
    moved = pl.pallas_call(
        move_kernel,
        out_shape=pltpu.VMEM((3, 16, 8) + brick, bf16),
        in_specs=[pl.BlockSpec(memory_space=pltpu.SMEM), any_space, any_space, any_space],
        out_specs=pl.BlockSpec(memory_space=pltpu.VMEM),
        scratch_shapes=scratch,
        compiler_params=pltpu.CompilerParams(
            collective_id=2, has_side_effects=True, vmem_limit_bytes=51 * 2**20
        ),
        name="move",
    )(index, gate, up, down)

    mine = lax.dynamic_slice(low, ((g // 2) * 8,), (8,))
    return pl.pallas_call(
        scale_kernel,
        in_specs=[pl.BlockSpec(memory_space=pltpu.SMEM), pl.BlockSpec(memory_space=pltpu.VMEM)],
        out_specs=[any_space, pl.BlockSpec(memory_space=pltpu.VMEM)],
        out_shape=[
            jax.ShapeDtypeStruct((3, 1, 1, 8, columns, 16 * BLOCK), bf16),
            jax.ShapeDtypeStruct((3, 1, 1, 16, hidden), jnp.float32),
        ],
        scratch_shapes=[pltpu.VMEM((3, 8, columns, 16 * BLOCK), bf16), pltpu.VMEM((8, 16, columns), jnp.float32), dma((3, 8))],
        compiler_params=pltpu.CompilerParams(vmem_limit_bytes=20 * 2**20),
        name="scale",
    )(mine, moved)


def per_device(gate, up, down, source_order, target_order):
    slots, rows, hidden = gate.shape
    columns = hidden // 8
    tile = (BLOCK, hidden)
    brick = (columns, BLOCK)
    bf16, f32 = jnp.bfloat16, jnp.float32
    dma = pltpu.SemaphoreType.DMA
    any_space = pl.BlockSpec(memory_space=pl.ANY)
    smem = pl.BlockSpec(memory_space=pltpu.SMEM)
    vmem = pl.BlockSpec(memory_space=pltpu.VMEM)
    results = [
        jax.ShapeDtypeStruct((3, 1, 1, 8, columns, 16 * BLOCK), bf16),
        jax.ShapeDtypeStruct((3, 1, 1, 16, hidden), f32),
    ]

    table, level = pl.pallas_call(
        plan_kernel,
        out_shape=[
            jax.ShapeDtypeStruct((16, 128), jnp.int32),
            jax.ShapeDtypeStruct((1,), jnp.int32),
        ],
        in_specs=[vmem, vmem],
        out_specs=[vmem, smem],
        name="plan",
    )(source_order[None, :], target_order[None, :])

    def direct(room, number, table, gate, up, down, source_order, target_order):
        scratch = (
            [pltpu.VMEM((3, 4) + tile, bf16)] * 3
            + [pltpu.VMEM((3, 4) + tile, bf16)]
            + [pltpu.VMEM((16, 8) + brick, bf16)] * 3
            + [pltpu.VMEM((128,) + brick, bf16)] * 3
            + [pltpu.VMEM((2, 3, max(room), 2) + brick, bf16)] * 2
            + [pltpu.VMEM((2, 3, max(room), 2) + brick, bf16)] * 3
            + [pltpu.VMEM((8, 16, columns), f32)]
            + [dma((3,)), dma((3,)), dma((3, 3)), dma((3,)), dma((3, 7))]
            + [dma((3, 2, 3)), dma((3, 2, 3)), dma((3,)), dma((3, 2, 3))]
        )
        moved, early = pl.pallas_call(
            functools.partial(direct_kernel, room),
            out_shape=[pltpu.VMEM((3, 2, 4, 2, 8) + brick, bf16), pltpu.VMEM((2, 16, hidden), f32)],
            in_specs=[smem, any_space, any_space, any_space],
            out_specs=[vmem, vmem],
            scratch_shapes=scratch,
            compiler_params=pltpu.CompilerParams(
                collective_id=number, has_side_effects=True, vmem_limit_bytes=50 * 2**20
            ),
            name="direct",
        )(table, gate, up, down)
        return pl.pallas_call(
            write_kernel,
            in_specs=[vmem, vmem],
            out_specs=[any_space, vmem],
            out_shape=results,
            scratch_shapes=[
                pltpu.VMEM((8, columns, 16 * BLOCK), bf16),
                pltpu.VMEM((8, 16, columns), f32),
                dma((2,)),
                dma((8,)),
            ],
            compiler_params=pltpu.CompilerParams(vmem_limit_bytes=12 * 2**20),
            name="write",
        )(moved, early)

    operands = (table, gate, up, down, source_order, target_order)
    ways = [functools.partial(direct, room, 3 + i) for i, room in enumerate(ROOMS)]
    return tuple(lax.switch(level[0], ways + [through], *operands))


def solution(mesh):
    placed = (P("grp", "sub", None), P("grp", "sub", None), P("grp", "sub", None), P(), P())
    return jax.shard_map(
        per_device,
        mesh=mesh,
        in_specs=placed,
        out_specs=(P(None, "grp", "sub", None, None, None), P(None, "grp", "sub", None, None)),
        check_vma=False,
    )
```

```python
import functools

import jax
import jax.numpy as jnp
from jax import lax
from jax.experimental import pallas as pl
from jax.experimental.pallas import tpu as pltpu
from jax.sharding import PartitionSpec as P

BLOCK = 128
EPS = 1e-06
MESH = pl.DeviceIdType.MESH
MATS = 3
HOPS = (1, 3, 2)
ROOMS = ((14, 6), (15, 7), (16, 8))


def device(x, z, s8):
    return ((x * 4 + z) * 2 + s8 // 4, s8 % 4)


def flip(a, b):
    low = (a + b) % 2
    high = (a // 2 + b // 2) % 2
    return high * 2 + low


def place():
    g = lax.axis_index("grp")
    q = lax.axis_index("sub")
    return g // 8, (g // 2) % 4, g % 2, q


def greet(partners):
    barrier = pltpu.get_barrier_semaphore()
    for partner in partners:
        pl.semaphore_signal(barrier, inc=1, device_id=partner, device_id_type=MESH)
    pl.semaphore_wait(barrier, len(partners))


def drain(ref, sem):
    pltpu.make_async_copy(ref, ref, sem).wait()


def crossings(s8):
    return [flip((s8 // 4) * 2 + (s8 // 2) % 2, r // 2) * 2 + (s8 + r) % 2 for r in range(8)]


def window(ahead, across, behind, most, through_most):
    low = jnp.maximum(jnp.maximum(across - through_most, across + behind - most), 0)
    high = jnp.minimum(jnp.minimum(across, through_most), most - ahead)
    return low, high


def plan_kernel(source_ref, target_ref, table_ref, level_ref):
    x, z, _, _ = place()
    f32, i32 = jnp.float32, jnp.int32
    shape = (128, 128)
    row = lax.broadcasted_iota(i32, shape, 0)
    lane = lax.broadcasted_iota(i32, shape, 1)
    source = jnp.broadcast_to(source_ref[...].astype(f32), shape).T
    target = jnp.broadcast_to(target_ref[...].astype(f32), shape)
    found = jnp.where(source == target, lane.astype(f32), 0.0)
    to = jnp.broadcast_to(jnp.sum(found, axis=1, keepdims=True), shape).astype(i32)
    x_to, z_to = to // 32, (to // 8) % 4
    x_at, z_at = row // 32, (row // 8) % 4
    inner = ((row // 4) % 2) * 32 + row % 4

    def down(values):
        return jnp.sum(values.astype(f32), axis=0, keepdims=True).astype(i32)

    kinds = []
    misfit = [jnp.zeros(shape, f32)] * len(ROOMS)
    for kind in range(2):
        at, end = (x_at, x_to) if kind == 0 else (z_at, z_to)
        away = (end - at + 4) % 4
        at_lane, away_lane = at.astype(f32).T, away.astype(f32).T
        near = at_lane == at.astype(f32)

        def count(which):
            return jnp.broadcast_to(
                jnp.sum(jnp.where(which, 1.0, 0.0), axis=1, keepdims=True), shape
            ).astype(i32)

        rank = count(near & (away_lane == away.astype(f32)) & (lane < row))
        ahead, across, behind = (count(near & (away_lane == float(d))) for d in (1, 2, 3))
        kinds.append((at, away, rank, ahead, across, behind))
        for i, (most, through_most) in enumerate(ROOMS):
            low, high = window(ahead, across, behind, most, through_most)
            misfit[i] = jnp.maximum(misfit[i], jnp.where(low > high, 1.0, 0.0))
    level = jnp.int32(0)
    for bad in misfit:
        level += jnp.max(bad).astype(i32)
    level_ref[0] = level
    most, through_most = jnp.int32(ROOMS[-1][0]), jnp.int32(ROOMS[-1][1])
    for i in reversed(range(len(ROOMS) - 1)):
        most = jnp.where(level <= i, ROOMS[i][0], most)
        through_most = jnp.where(level <= i, ROOMS[i][1], through_most)

    table_ref[8:16, :] = jnp.zeros((8, 128), i32)
    for kind in range(2):
        at, away, rank, ahead, across, behind = kinds[kind]
        low, high = window(ahead, across, behind, most, through_most)
        right = jnp.minimum(jnp.maximum((across + behind - ahead + 64) // 2 - 32, low), high)
        back = jnp.where((away == 1) | ((away == 2) & (rank < right)), 0, 1)
        slot = jnp.where(
            away == 1,
            right + rank,
            jnp.where(away == 3, across - right + rank, jnp.where(rank < right, rank, rank - right)),
        )
        index = kind * 64 + inner + (z_at if kind == 0 else x_at) * 4
        mine = x if kind == 0 else z
        sent = (at == mine) & (away > 0) & (back == lane // 32) & (slot == lane % 32)
        step = lane // 8
        if kind == 0:
            place_here = (x * 4 + (z + step) % 4) * 8 + lane % 8
        else:
            place_here = (((x + step) % 4) * 4 + z) * 8 + lane % 8
        got = (to == place_here) & (lane < 32)
        moved = got & (away > 0)
        base = kind * 5
        table_ref[base : base + 1, :] = down(jnp.where(sent, index, 0))
        table_ref[base + 1 : base + 2, :] = down(jnp.where(got & (away == 0), index, 0))
        table_ref[base + 2 : base + 3, :] = down(jnp.where(moved, back, 0))
        table_ref[base + 3 : base + 4, :] = down(
            jnp.where(moved, slot + jnp.where(away == 2, 64, 0), 0)
        )
        table_ref[base + 4 : base + 5, :] = down(jnp.where(got & (away == 0), 1, 0))


def quantize(load, store, columns):
    lane = lax.broadcasted_iota(jnp.int32, (columns, BLOCK), 1)
    seen = jnp.zeros((columns, BLOCK), jnp.float32)
    for b in range(16):
        values = load(b).astype(jnp.float32)
        scale = jnp.max(jnp.abs(values), axis=1, keepdims=True) + EPS
        store(b, (values * (1.0 / scale)).astype(jnp.bfloat16))
        seen = jnp.where(lane == b, scale, seen)
    return seen.T[:16]


def direct_kernel(room, table, gate, up, down, out, scales, *scratch):
    first = scratch[0:3]
    own = scratch[3]
    turned = scratch[4:7]
    middle = scratch[7:10]
    packs = scratch[10:12]
    landed = scratch[12:15]
    found = scratch[15]
    own_sem, first_send, first_recv, y_send, y_recv = scratch[16:21]
    direct_send, direct_recv, onward_send, onward_recv, last_send, last_recv = scratch[21:27]
    weights = (gate, up, down)
    most, through_most = room
    parts = ((0, through_most), (through_most, most - through_most))

    x, z, yl, q = place()
    core = q % 2
    s8 = yl * 4 + q
    units, columns = turned[0].shape[1], turned[0].shape[2]

    def pick(a, b):
        return jnp.where(core == 0, a, b)

    x_to = [device((x + d) % 4, z, s8) for d in range(4)]
    z_to = [device(x, (z + d) % 4, s8) for d in range(4)]
    s8_to = crossings(s8)
    y_to = [device(x, z, s) for s in s8_to]
    greet(x_to[1:] + z_to[1:] + y_to[1:])

    spot = pick(z, x)

    def rows(m, d):
        block = (spot + d) % 4
        return weights[m].at[:, pl.ds(pl.multiple_of(block * BLOCK, BLOCK), BLOCK), :]

    def first_copy(m, d):
        return pltpu.make_async_remote_copy(
            src_ref=rows(m, d),
            dst_ref=first[m].at[d - 1],
            send_sem=first_send.at[m],
            recv_sem=first_recv.at[m, d - 1],
            device_id=tuple(pick(a, b) for a, b in zip(z_to[d], x_to[d])),
            device_id_type=MESH,
        )

    def own_copy(m):
        return pltpu.make_async_copy(rows(m, 0), own.at[m], own_sem.at[m])

    slot = (core * 4 + yl * 2 + q // 2) * 16

    def origin(d):
        return ((spot + 4 - d) % 4) * 4

    def y_copy(m, d, r):
        return pltpu.make_async_remote_copy(
            src_ref=turned[m].at[pl.ds(origin(d), 4), s8_to[r]],
            dst_ref=middle[m].at[pl.ds(slot + origin(d), 4)],
            send_sem=y_send.at[m],
            recv_sem=y_recv.at[m, r - 1],
            device_id=y_to[r],
            device_id_type=MESH,
        )

    def direct_copy(m, kind, back, part):
        start, count = parts[part]
        return pltpu.make_async_remote_copy(
            src_ref=packs[m % 2].at[kind, back, pl.ds(start, count)],
            dst_ref=landed[m].at[kind, back, pl.ds(start, count)],
            send_sem=direct_send.at[m, kind, back, part],
            recv_sem=direct_recv.at[m, kind, back, part],
            device_id=(x_to, z_to)[kind][(1, 3)[back]],
            device_id_type=MESH,
        )

    def onward_copy(m, kind, back):
        return pltpu.make_async_remote_copy(
            src_ref=landed[m].at[kind, back, pl.ds(0, through_most)],
            dst_ref=landed[m].at[kind, back, pl.ds(most, through_most)],
            send_sem=onward_send.at[m, kind, back],
            recv_sem=onward_recv.at[m, kind, back],
            device_id=(x_to, z_to)[kind][(1, 3)[back]],
            device_id_type=MESH,
        )

    ways = [(kind, back) for back in range(2) for kind in range(2)]

    def last_copy(m, kind, d):
        return pltpu.make_async_remote_copy(
            src_ref=turned[m].at[pl.ds((kind * 3 + d - 1) * 2, 2)],
            dst_ref=out.at[m, kind, (z, x)[kind]],
            send_sem=last_send.at[m],
            recv_sem=last_recv.at[m, kind, d - 1],
            device_id=(z_to, x_to)[kind][d],
            device_id_type=MESH,
        )

    def start(m):
        for d in HOPS:
            first_copy(m, d).start()
        own_copy(m).start()

    def turn(m, d):
        if d:
            first_copy(m, d).wait_recv()
            tiles = first[m].at[d - 1]
        else:
            own_copy(m).wait()
            tiles = own.at[m]

        def one(i, carry):
            turned[m][origin(d) + i] = tiles[i].T.reshape(units, columns, BLOCK)
            return carry

        lax.fori_loop(0, 4, one, 0)
        for r in (2, 4, 6, 3, 5, 7, 1):
            y_copy(m, d, r).start()
        middle[m][pl.ds(slot + origin(d), 4)] = turned[m][pl.ds(origin(d), 4), s8]

    def gather(m):
        for r in range(1, 8):
            drain(middle[m].at[pl.ds(0, 16)], y_recv.at[m, r - 1])
        if m == 2:
            for part in range(2):
                for kind, back in ways:
                    direct_copy(0, kind, back, part).wait_send()
        for part in range(2):
            for kind, back in ways:

                def one(r, carry):
                    slot_in = parts[part][0] + r
                    index = table[kind * 5, back * 32 + slot_in]
                    for half in range(2):
                        packs[m % 2][kind, back, slot_in, half] = middle[m][index + 16 * half]
                    return carry

                lax.fori_loop(0, parts[part][1], one, 0)
                direct_copy(m, kind, back, part).start()

    def relay(m):
        for kind, back in ways:
            direct_copy(m, kind, back, 0).wait_recv()
            onward_copy(m, kind, back).start()

    def spread(m):
        for kind, back in ways:
            direct_copy(m, kind, back, 1).wait_recv()
            onward_copy(m, kind, back).wait_recv()
        drain(turned[m].at[pl.ds(0, 14)], y_send.at[m])
        for d in HOPS + (0,):
            for kind in range(2):

                def one(k, carry):
                    spot_in = d * 8 + k
                    near = table[kind * 5 + 1, spot_in]
                    hop = table[kind * 5 + 2, spot_in]
                    rank = table[kind * 5 + 3, spot_in]
                    stay = table[kind * 5 + 4, spot_in] > 0
                    for half in range(2):
                        here = middle[m][near + 16 * half]
                        there = landed[m][kind, hop, rank % 64 + rank // 64 * most, half]
                        brick = lax.select(jnp.broadcast_to(stay, here.shape), here, there)
                        if d == 0:
                            out[m, kind, (z, x)[kind], half, k] = brick
                        else:
                            turned[m][(kind * 3 + d - 1) * 2 + half, k] = brick
                    return carry

                lax.fori_loop(0, 8, one, 0)
                if d:
                    last_copy(m, kind, d).start()

    def settle(m):
        for kind in range(2):
            for d in HOPS:
                last_copy(m, kind, d).wait_recv()
        if m == MATS - 1:
            return

        def one(k, carry):
            def load(b):
                return out[m, (b // 4) % 2, b % 4, b // 8, k]

            def store(b, brick):
                out[m, (b // 4) % 2, b % 4, b // 8, k] = brick

            found[k] = quantize(load, store, columns)
            return carry

        lax.fori_loop(0, 8, one, 0)
        scales[m] = jnp.concatenate([found[k] for k in range(8)], axis=1)

    for m in range(MATS):
        start(m)
    turn(0, 0)
    turn(1, 0)
    for d in HOPS:
        turn(0, d)
    for d in HOPS:
        turn(1, d)
    turn(2, 0)
    gather(0)
    for d in HOPS:
        turn(2, d)
    relay(0)
    gather(1)
    spread(0)
    relay(1)
    gather(2)
    spread(1)
    relay(2)
    settle(0)
    spread(2)
    settle(1)
    settle(2)

    for m in range(MATS):
        drain(first[m], first_send.at[m])
        for kind, back in ways:
            if m:
                for part in range(2):
                    direct_copy(m, kind, back, part).wait_send()
            onward_copy(m, kind, back).wait_send()
        drain(turned[m].at[pl.ds(0, 12)], last_send.at[m])


def write_kernel(moved, early, packed, scales, ready, found, early_sem, sem):
    columns = moved.shape[-2]
    last = MATS - 1

    def early_copy(m, k, b):
        return pltpu.make_async_copy(
            moved.at[m, (b // 4) % 2, b % 4, b // 8, k],
            packed.at[m, 0, 0, k, :, pl.ds(b * BLOCK, BLOCK)],
            early_sem.at[m],
        )

    def late_copy(k):
        return pltpu.make_async_copy(ready.at[k], packed.at[last, 0, 0, k], sem.at[k])

    for m in range(last):

        def issue(k, carry):
            for b in range(16):
                early_copy(m, k, b).start()
            return carry

        lax.fori_loop(0, 8, issue, 0)

    def one(k, carry):
        def load(b):
            return moved[last, (b // 4) % 2, b % 4, b // 8, k]

        def store(b, brick):
            ready[k, :, b * BLOCK : (b + 1) * BLOCK] = brick

        found[k] = quantize(load, store, columns)
        late_copy(k).start()
        return carry

    lax.fori_loop(0, 8, one, 0)
    for m in range(last):
        scales[m, 0, 0] = early[m]
    scales[last, 0, 0] = jnp.concatenate([found[k] for k in range(8)], axis=1)
    for m in range(last):
        drain(packed.at[m], early_sem.at[m])
    for k in range(8):
        late_copy(k).wait()


def move_kernel(index_ref, gate, up, down, out, *scratch):
    first = scratch[0:3]
    second = scratch[3:6]
    own = scratch[6]
    turned = scratch[7:10]
    middle = scratch[10:13]
    sorted_ = scratch[13:16]
    relay = scratch[16:19]
    own_sem, first_send, first_recv, second_send, second_recv = scratch[19:24]
    y_send, y_recv, third_send, third_recv, last_send, last_recv, keep_sem = scratch[24:31]
    weights = (gate, up, down)

    g = lax.axis_index("grp")
    q = lax.axis_index("sub")
    x, z, yl = g // 8, (g // 2) % 4, g % 2
    core = q % 2
    s8 = yl * 4 + q

    def device(xx, zz, ss):
        return ((xx * 4 + zz) * 2 + ss // 4, ss % 4)

    def pick(a, b):
        return jnp.where(core == 0, a, b)

    def flip(a, b):
        low = (a + b) % 2
        high = (a // 2 + b // 2) % 2
        return high * 2 + low

    x_to = [(x + d) % 4 for d in range(4)]
    z_to = [(z + d) % 4 for d in range(4)]
    x_from = [(x + 4 - d) % 4 for d in range(4)]
    z_from = [(z + 4 - d) % 4 for d in range(4)]
    dev1 = [device(pick(x, x_to[d]), pick(z_to[d], z), s8) for d in range(4)]
    dev2 = [device(pick(x_to[d], x), pick(z, z_to[d]), s8) for d in range(4)]
    s8_to = [(flip((s8 // 4) * 2 + (s8 // 2) % 2, r // 2)) * 2 + (s8 + r) % 2 for r in range(8)]
    dev_y = [device(x, z, s8_to[r]) for r in range(8)]

    barrier = pltpu.get_barrier_semaphore()
    partners = dev1[1:] + dev2[1:] + dev_y[1:]
    for partner in partners:
        pl.semaphore_signal(barrier, inc=1, device_id=partner, device_id_type=MESH)
    pl.semaphore_wait(barrier, len(partners))

    tile2 = [pick(flip(q, x_to[d]), z_to[d]) for d in range(4)]

    def source(m, d1, t):
        slot = pick(t, flip(q, x_to[d1]))
        block = pick(z_to[d1], t)
        return weights[m].at[slot, pl.ds(pl.multiple_of(block * BLOCK, BLOCK), BLOCK), :]

    def first_copy(m, d1, d2):
        t = tile2[d2]
        return pltpu.make_async_remote_copy(
            src_ref=source(m, d1, t),
            dst_ref=first[m].at[d1 - 1, t],
            send_sem=first_send.at[m],
            recv_sem=first_recv.at[m, d1 - 1, t],
            device_id=dev1[d1],
            device_id_type=MESH,
        )

    def second_copy(m, d1, d2):
        t = tile2[d2]
        return pltpu.make_async_remote_copy(
            src_ref=source(m, 0, t) if d1 == 0 else first[m].at[d1 - 1, t],
            dst_ref=second[m].at[d2 - 1, d1],
            send_sem=second_send.at[m],
            recv_sem=second_recv.at[m, d2 - 1, d1],
            device_id=dev2[d2],
            device_id_type=MESH,
        )

    def own_copy(m):
        return pltpu.make_async_copy(source(m, 0, tile2[0]), own.at[m], own_sem.at[m])

    def start_first(m):
        for d2 in (1, 3, 2, 0):
            for d1 in HOPS:
                first_copy(m, d1, d2).start()
        for d2 in HOPS:
            second_copy(m, 0, d2).start()
        own_copy(m).start()

    def forward(m):
        for d2 in (1, 3, 2, 0):
            for d1 in HOPS:
                first_copy(m, d1, d2).wait_recv()
                if d2:
                    second_copy(m, d1, d2).start()

    units, columns = turned[0].shape[1], turned[0].shape[2]

    def y_copy(m, r):
        return pltpu.make_async_remote_copy(
            src_ref=turned[m].at[:, s8_to[r]],
            dst_ref=middle[m].at[pl.ds(s8 * 16, 16)],
            send_sem=y_send.at[m],
            recv_sem=y_recv.at[m, r - 1],
            device_id=dev_y[r],
            device_id_type=MESH,
        )

    def place_of(d1, d2):
        return pick(x_from[d2] * 4 + z_from[d1], x_from[d1] * 4 + z_from[d2])

    def turn_and_cross(m):
        own_copy(m).wait()

        def turn(tile, place):
            turned[m][place] = tile.T.reshape(units, columns, BLOCK)

        turn(own[m], place_of(0, 0))
        for d1 in HOPS:
            turn(first[m][d1 - 1, tile2[0]], place_of(d1, 0))
        for d1 in (0,) + HOPS:
            for d2 in HOPS:
                second_copy(m, d1, d2).wait_recv()
                turn(second[m][d2 - 1, d1], place_of(d1, d2))
        for r in range(1, 8):
            y_copy(m, r).start()
        middle[m][pl.ds(s8 * 16, 16)] = turned[m][:, s8]

    def third_copy(m, d1, t):
        return pltpu.make_async_remote_copy(
            src_ref=sorted_[m].at[pick(t, x_to[d1]), pick(z_to[d1], t)],
            dst_ref=relay[m].at[d1 - 1, t],
            send_sem=third_send.at[m],
            recv_sem=third_recv.at[m, d1 - 1, t],
            device_id=dev1[d1],
            device_id_type=MESH,
        )

    def last_source(m, d1, d2):
        t = pick(x_to[d2], z_to[d2])
        if d1 == 0:
            return sorted_[m].at[pick(t, x), pick(z, t)]
        return relay[m].at[d1 - 1, t]

    def last_place(m, d1):
        return out.at[m, pick(x * 4 + z_from[d1], x_from[d1] * 4 + z)]

    def last_copy(m, d1, d2):
        return pltpu.make_async_remote_copy(
            src_ref=last_source(m, d1, d2),
            dst_ref=last_place(m, d1),
            send_sem=last_send.at[m],
            recv_sem=last_recv.at[m],
            device_id=dev2[d2],
            device_id_type=MESH,
        )

    def keep_copy(m, d1):
        return pltpu.make_async_copy(last_source(m, d1, 0), last_place(m, d1), keep_sem.at[m, d1])

    def third_tile(d2):
        return pick(x_to[d2], z_to[d2])

    def permute(m):
        for r in range(1, 8):
            y_copy(m, r).wait_recv()

        def step(t, carry):
            for k in range(8):
                sorted_[m][t // 4, t % 4, k] = middle[m][index_ref[t * 8 + k]]
            return carry

        lax.fori_loop(0, 16, step, 0)
        for d2 in (1, 3, 2, 0):
            for d1 in HOPS:
                third_copy(m, d1, third_tile(d2)).start()
        for d2 in HOPS:
            last_copy(m, 0, d2).start()
        keep_copy(m, 0).start()

    def finish(m):
        for d2 in (1, 3, 2, 0):
            for d1 in HOPS:
                third_copy(m, d1, third_tile(d2)).wait_recv()
                if d2:
                    last_copy(m, d1, d2).start()
                else:
                    keep_copy(m, d1).start()

    start_first(0)
    start_first(1)
    start_first(2)
    forward(0)
    forward(1)
    turn_and_cross(0)
    forward(2)
    turn_and_cross(1)
    permute(0)
    turn_and_cross(2)
    finish(0)
    permute(1)
    finish(1)
    permute(2)
    finish(2)

    def drain(ref, sem):
        pltpu.make_async_copy(ref, ref, sem).wait()

    for m in range(MATS):
        drain(first[m], first_send.at[m])
        drain(second[m], second_send.at[m])
        drain(middle[m].at[pl.ds(0, 112)], y_send.at[m])
        drain(relay[m], third_send.at[m])
        drain(relay[m], last_send.at[m])
        drain(relay[m], last_recv.at[m])
        for d1 in range(4):
            keep_copy(m, d1).wait()


def scale_kernel(low_ref, moved, packed, scales, ready, found, sem):
    columns = moved.shape[3]
    lane = lax.broadcasted_iota(jnp.int32, (columns, BLOCK), 1)

    def out_copy(m, k):
        return pltpu.make_async_copy(ready.at[m, k], packed.at[m, 0, 0, k], sem.at[m, k])

    for m in range(MATS):

        def step(k, carry):
            low = low_ref[k]
            seen = jnp.zeros((columns, BLOCK), jnp.float32)
            for b in range(16):
                place = ((b // 4) ^ low) * 4 + b % 4
                values = moved[m, place, k].astype(jnp.float32)
                scale = jnp.max(jnp.abs(values), axis=1, keepdims=True) + EPS
                ready[m, k, :, b * BLOCK : (b + 1) * BLOCK] = (values * (1.0 / scale)).astype(jnp.bfloat16)
                seen = jnp.where(lane == b, scale, seen)
            found[k] = seen.T[:16]
            out_copy(m, k).start()
            return carry

        lax.fori_loop(0, 8, step, 0)
        scales[m, 0, 0] = jnp.concatenate([found[k] for k in range(8)], axis=1)

    for m in range(MATS):
        for k in range(8):
            out_copy(m, k).wait()


def through(table, gate, up, down, source_order, target_order):
    slots, rows, hidden = gate.shape
    columns = hidden // 8
    experts = source_order.shape[0]
    matches = (source_order[None, :] == target_order[:, None]).astype(jnp.int32)
    picked = jnp.sum(matches * jnp.arange(experts, dtype=jnp.int32)[None, :], axis=1)
    g = lax.axis_index("grp")
    x = g // 8
    col, yl, low = picked // 8, (picked // 4) % 2, picked % 4
    index = (yl * 4 + (low ^ x)) * 16 + col

    tile = (BLOCK, hidden)
    brick = (columns, BLOCK)
    bf16 = jnp.bfloat16
    dma = pltpu.SemaphoreType.DMA
    any_space = pl.BlockSpec(memory_space=pl.ANY)
    scratch = (
        [pltpu.VMEM((3, 4) + tile, bf16)] * 3
        + [pltpu.VMEM((3, 4) + tile, bf16)] * 3
        + [pltpu.VMEM((3,) + tile, bf16)]
        + [pltpu.VMEM((16, 8) + brick, bf16)] * 3
        + [pltpu.VMEM((128,) + brick, bf16)] * 3
        + [pltpu.VMEM((4, 4, 8) + brick, bf16)] * 3
        + [pltpu.VMEM((3, 4, 8) + brick, bf16)] * 3
        + [dma((3,)), dma((3,)), dma((3, 3, 4)), dma((3,)), dma((3, 3, 4))]
        + [dma((3,)), dma((3, 7)), dma((3,)), dma((3, 3, 4)), dma((3,)), dma((3,)), dma((3, 4))]
    )
    moved = pl.pallas_call(
        move_kernel,
        out_shape=pltpu.VMEM((3, 16, 8) + brick, bf16),
        in_specs=[pl.BlockSpec(memory_space=pltpu.SMEM), any_space, any_space, any_space],
        out_specs=pl.BlockSpec(memory_space=pltpu.VMEM),
        scratch_shapes=scratch,
        compiler_params=pltpu.CompilerParams(
            collective_id=2, has_side_effects=True, vmem_limit_bytes=51 * 2**20
        ),
        name="move",
    )(index, gate, up, down)

    mine = lax.dynamic_slice(low, ((g // 2) * 8,), (8,))
    return pl.pallas_call(
        scale_kernel,
        in_specs=[pl.BlockSpec(memory_space=pltpu.SMEM), pl.BlockSpec(memory_space=pltpu.VMEM)],
        out_specs=[any_space, pl.BlockSpec(memory_space=pltpu.VMEM)],
        out_shape=[
            jax.ShapeDtypeStruct((3, 1, 1, 8, columns, 16 * BLOCK), bf16),
            jax.ShapeDtypeStruct((3, 1, 1, 16, hidden), jnp.float32),
        ],
        scratch_shapes=[pltpu.VMEM((3, 8, columns, 16 * BLOCK), bf16), pltpu.VMEM((8, 16, columns), jnp.float32), dma((3, 8))],
        compiler_params=pltpu.CompilerParams(vmem_limit_bytes=20 * 2**20),
        name="scale",
    )(mine, moved)


def per_device(gate, up, down, source_order, target_order):
    slots, rows, hidden = gate.shape
    columns = hidden // 8
    tile = (BLOCK, hidden)
    brick = (columns, BLOCK)
    bf16, f32 = jnp.bfloat16, jnp.float32
    dma = pltpu.SemaphoreType.DMA
    any_space = pl.BlockSpec(memory_space=pl.ANY)
    smem = pl.BlockSpec(memory_space=pltpu.SMEM)
    vmem = pl.BlockSpec(memory_space=pltpu.VMEM)
    results = [
        jax.ShapeDtypeStruct((3, 1, 1, 8, columns, 16 * BLOCK), bf16),
        jax.ShapeDtypeStruct((3, 1, 1, 16, hidden), f32),
    ]

    table, level = pl.pallas_call(
        plan_kernel,
        out_shape=[
            jax.ShapeDtypeStruct((16, 128), jnp.int32),
            jax.ShapeDtypeStruct((1,), jnp.int32),
        ],
        in_specs=[vmem, vmem],
        out_specs=[vmem, smem],
        name="plan",
    )(source_order[None, :], target_order[None, :])

    def direct(room, number, table, gate, up, down, source_order, target_order):
        scratch = (
            [pltpu.VMEM((3, 4) + tile, bf16)] * 3
            + [pltpu.VMEM((3, 4) + tile, bf16)]
            + [pltpu.VMEM((16, 8) + brick, bf16)] * 3
            + [pltpu.VMEM((128,) + brick, bf16)] * 3
            + [pltpu.VMEM((2, 2, room[0], 2) + brick, bf16)] * 2
            + [pltpu.VMEM((2, 2, room[0] + room[1], 2) + brick, bf16)] * 3
            + [pltpu.VMEM((8, 16, columns), f32)]
            + [dma((3,)), dma((3,)), dma((3, 3)), dma((3,)), dma((3, 7))]
            + [dma((3, 2, 2, 2))] * 2
            + [dma((3, 2, 2))] * 2
            + [dma((3,)), dma((3, 2, 3))]
        )
        moved, early = pl.pallas_call(
            functools.partial(direct_kernel, room),
            out_shape=[pltpu.VMEM((3, 2, 4, 2, 8) + brick, bf16), pltpu.VMEM((2, 16, hidden), f32)],
            in_specs=[smem, any_space, any_space, any_space],
            out_specs=[vmem, vmem],
            scratch_shapes=scratch,
            compiler_params=pltpu.CompilerParams(
                collective_id=number, has_side_effects=True, vmem_limit_bytes=50 * 2**20
            ),
            name="direct",
        )(table, gate, up, down)
        return pl.pallas_call(
            write_kernel,
            in_specs=[vmem, vmem],
            out_specs=[any_space, vmem],
            out_shape=results,
            scratch_shapes=[
                pltpu.VMEM((8, columns, 16 * BLOCK), bf16),
                pltpu.VMEM((8, 16, columns), f32),
                dma((2,)),
                dma((8,)),
            ],
            compiler_params=pltpu.CompilerParams(vmem_limit_bytes=12 * 2**20),
            name="write",
        )(moved, early)

    operands = (table, gate, up, down, source_order, target_order)
    ways = [functools.partial(direct, room, 3 + i) for i, room in enumerate(ROOMS)]
    return tuple(lax.switch(level[0], ways + [through], *operands))


def solution(mesh):
    placed = (P("grp", "sub", None), P("grp", "sub", None), P("grp", "sub", None), P(), P())
    return jax.shard_map(
        per_device,
        mesh=mesh,
        in_specs=placed,
        out_specs=(P(None, "grp", "sub", None, None, None), P(None, "grp", "sub", None, None)),
        check_vma=False,
    )
```

```python
import functools

import jax
import jax.numpy as jnp
from jax import lax
from jax.experimental import pallas as pl
from jax.experimental.pallas import tpu as pltpu
from jax.sharding import PartitionSpec as P

BLOCK = 128
EPS = 1e-06
MESH = pl.DeviceIdType.MESH
MATS = 3
HOPS = (1, 3, 2)
ROOMS = ((13, 6), (14, 6), (15, 7), (16, 8))


def device(x, z, s8):
    return ((x * 4 + z) * 2 + s8 // 4, s8 % 4)


def flip(a, b):
    low = (a + b) % 2
    high = (a // 2 + b // 2) % 2
    return high * 2 + low


def place():
    g = lax.axis_index("grp")
    q = lax.axis_index("sub")
    return g // 8, (g // 2) % 4, g % 2, q


def greet(partners):
    barrier = pltpu.get_barrier_semaphore()
    for partner in partners:
        pl.semaphore_signal(barrier, inc=1, device_id=partner, device_id_type=MESH)
    pl.semaphore_wait(barrier, len(partners))


def drain(ref, sem):
    pltpu.make_async_copy(ref, ref, sem).wait()


def crossings(s8):
    return [flip((s8 // 4) * 2 + (s8 // 2) % 2, r // 2) * 2 + (s8 + r) % 2 for r in range(8)]


def window(ahead, across, behind, most, through_most):
    low = jnp.maximum(jnp.maximum(across - through_most, across + behind - most), 0)
    high = jnp.minimum(jnp.minimum(across, through_most), most - ahead)
    return low, high


def plan_kernel(source_ref, target_ref, table_ref, level_ref):
    x, z, _, _ = place()
    f32, i32 = jnp.float32, jnp.int32
    square = (128, 128)
    row = lax.broadcasted_iota(i32, square, 0)
    lane = lax.broadcasted_iota(i32, square, 1)
    p = lax.broadcasted_iota(i32, (1, 128), 1)

    def upright(values):
        return jnp.broadcast_to(values.astype(f32), square).T

    def total(values):
        return jnp.sum(values, axis=0, keepdims=True).astype(i32)

    wanted = upright(target_ref[...]) == source_ref[...].astype(f32)
    to = total(jnp.where(wanted, row.astype(f32), 0.0))
    to_row = upright(to).astype(i32)

    def plane(slot, kind):
        return slot // 32 if kind == 0 else (slot // 8) % 4

    kinds = []
    worst = jnp.zeros((1, 128), i32)
    for kind in range(2):
        at, end = plane(p, kind), plane(to, kind)
        away = (end - at + 4) % 4
        key_row = plane(row, kind) * 4 + plane(to_row, kind)

        def count(which):
            return total(jnp.where(which, 1.0, 0.0))

        rank = count((key_row == at * 4 + end) & (row < lane))
        ahead, across, behind = (count(key_row == at * 4 + (at + d) % 4) for d in (1, 2, 3))
        kinds.append((at, away, rank, ahead, across, behind))
        misfit = jnp.zeros((1, 128), i32)
        for most, through_most in ROOMS:
            low, high = window(ahead, across, behind, most, through_most)
            misfit += jnp.where(low > high, 1, 0)
        worst = jnp.maximum(worst, misfit)
    level = jnp.max(worst.astype(f32)).astype(i32)
    level_ref[0] = level
    most, through_most = jnp.int32(ROOMS[-1][0]), jnp.int32(ROOMS[-1][1])
    for i in reversed(range(len(ROOMS) - 1)):
        most = jnp.where(level <= i, ROOMS[i][0], most)
        through_most = jnp.where(level <= i, ROOMS[i][1], through_most)

    table_ref[...] = jnp.zeros((8, 128), i32)
    for kind in range(2):
        at, away, rank, ahead, across, behind = kinds[kind]
        low, high = window(ahead, across, behind, most, through_most)
        right = jnp.minimum(jnp.maximum((across + behind - ahead + 64) // 2 - 32, low), high)
        back = jnp.where((away == 1) | ((away == 2) & (rank < right)), 0, 1)
        slot = jnp.where(
            away == 1,
            right + rank,
            jnp.where(away == 3, across - right + rank, jnp.where(rank < right, rank, rank - right)),
        )
        index = kind * 64 + ((p // 4) % 2) * 32 + plane(p, 1 - kind) * 4 + p % 4
        mine = (x, z)[kind]
        send = jnp.where((at == mine) & (away > 0), back * 32 + slot, 127)
        step = (plane(to, 1 - kind) - (z, x)[kind] + 4) % 4
        receive = jnp.where(plane(to, kind) == mine, step * 8 + to % 8, 127)
        code = jnp.where(
            away == 0,
            32768 + index,
            back * 16384 + (slot + jnp.where(away == 2, 64, 0)) * 128,
        )
        for i, (spot, value) in enumerate(((send, index), (receive, code))):
            joint = upright(spot * 65536 + value).astype(i32)
            here = (joint // 65536 == lane) & (lane < 127)
            found = total(jnp.where(here, (joint % 65536).astype(f32), 0.0))
            table_ref[kind * 2 + i : kind * 2 + i + 1, :] = found


def quantize(load, store, columns):
    lane = lax.broadcasted_iota(jnp.int32, (columns, BLOCK), 1)
    seen = jnp.zeros((columns, BLOCK), jnp.float32)
    for b in range(16):
        values = load(b).astype(jnp.float32)
        scale = jnp.max(jnp.abs(values), axis=1, keepdims=True) + EPS
        store(b, (values * (1.0 / scale)).astype(jnp.bfloat16))
        seen = jnp.where(lane == b, scale, seen)
    return seen.T[:16]


def direct_kernel(room, table, gate, up, down, out, scales, *scratch):
    first = scratch[0:3]
    turned = scratch[3:6]
    middle = scratch[6:9]
    packs = scratch[9:11]
    landed = scratch[11:14]
    found = scratch[14]
    first_send, first_recv, y_send, y_recv = scratch[15:19]
    direct_send, direct_recv, onward_send, onward_recv, last_send, last_recv = scratch[19:25]
    weights = (gate, up, down)
    most, through_most = room
    parts = ((0, through_most), (through_most, most - through_most))

    x, z, yl, q = place()
    core = q % 2
    s8 = yl * 4 + q
    units, columns = turned[0].shape[1], turned[0].shape[2]

    def pick(a, b):
        return jnp.where(core == 0, a, b)

    x_to = [device((x + d) % 4, z, s8) for d in range(4)]
    z_to = [device(x, (z + d) % 4, s8) for d in range(4)]
    s8_to = crossings(s8)
    y_to = [device(x, z, s) for s in s8_to]
    greet(x_to[1:] + z_to[1:] + y_to[1:])

    spot = pick(z, x)

    def rows(m, d):
        block = (spot + d) % 4
        return weights[m].at[:, pl.ds(pl.multiple_of(block * BLOCK, BLOCK), BLOCK), :]

    def first_copy(m, d):
        return pltpu.make_async_remote_copy(
            src_ref=rows(m, d),
            dst_ref=first[m].at[d],
            send_sem=first_send.at[m],
            recv_sem=first_recv.at[m, d],
            device_id=tuple(pick(a, b) for a, b in zip(z_to[d], x_to[d])),
            device_id_type=MESH,
        )

    def own_copy(m):
        return pltpu.make_async_copy(rows(m, 0), first[m].at[0], first_recv.at[m, 0])

    slot = (core * 4 + yl * 2 + q // 2) * 16

    def origin(d):
        return ((spot + 4 - d) % 4) * 4

    def y_copy(m, d, r):
        return pltpu.make_async_remote_copy(
            src_ref=turned[m].at[pl.ds(origin(d), 4), s8_to[r]],
            dst_ref=middle[m].at[pl.ds(slot + origin(d), 4)],
            send_sem=y_send.at[m],
            recv_sem=y_recv.at[m, r - 1],
            device_id=y_to[r],
            device_id_type=MESH,
        )

    def direct_copy(m, kind, back, part):
        start, count = parts[part]
        return pltpu.make_async_remote_copy(
            src_ref=packs[m % 2].at[kind, back, pl.ds(start, count)],
            dst_ref=landed[m].at[kind, back, pl.ds(start, count)],
            send_sem=direct_send.at[m, kind, back, part],
            recv_sem=direct_recv.at[m, kind, back, part],
            device_id=(x_to, z_to)[kind][(1, 3)[back]],
            device_id_type=MESH,
        )

    def onward_copy(m, kind, back):
        return pltpu.make_async_remote_copy(
            src_ref=landed[m].at[kind, back, pl.ds(0, through_most)],
            dst_ref=landed[m].at[kind, back, pl.ds(most, through_most)],
            send_sem=onward_send.at[m, kind, back],
            recv_sem=onward_recv.at[m, kind, back],
            device_id=(x_to, z_to)[kind][(1, 3)[back]],
            device_id_type=MESH,
        )

    ways = [(kind, back) for back in range(2) for kind in range(2)]

    def last_copy(m, kind, d):
        return pltpu.make_async_remote_copy(
            src_ref=turned[m].at[pl.ds((kind * 3 + d - 1) * 2, 2)],
            dst_ref=out.at[m, kind, (z, x)[kind]],
            send_sem=last_send.at[m],
            recv_sem=last_recv.at[m, kind, d - 1],
            device_id=(z_to, x_to)[kind][d],
            device_id_type=MESH,
        )

    def start(m):
        for d in HOPS:
            first_copy(m, d).start()
        own_copy(m).start()

    def turn(m, low, high):
        def group(step, carry):
            d = flip(step, step // 2)
            drain(first[m].at[d], first_recv.at[m, d])

            def one(i, inner):
                turned[m][origin(d) + i] = first[m][d, i].T.reshape(units, columns, BLOCK)
                return inner

            lax.fori_loop(0, 4, one, 0)
            for r in (2, 4, 6, 3, 5, 7, 1):
                y_copy(m, d, r).start()
            middle[m][pl.ds(slot + origin(d), 4)] = turned[m][pl.ds(origin(d), 4), s8]
            return carry

        lax.fori_loop(low, high, group, 0)

    def gather(m):
        for r in range(1, 8):
            drain(middle[m].at[pl.ds(0, 16)], y_recv.at[m, r - 1])
        if m == 2:
            for part in range(2):
                for kind, back in ways:
                    direct_copy(0, kind, back, part).wait_send()
        for part in range(2):
            for kind, back in ways:

                def one(r, carry):
                    slot_in = parts[part][0] + r
                    index = table[kind * 2, back * 32 + slot_in]
                    for half in range(2):
                        packs[m % 2][kind, back, slot_in, half] = middle[m][index + 16 * half]
                    return carry

                lax.fori_loop(0, parts[part][1], one, 0)
                direct_copy(m, kind, back, part).start()

    def relay(m):
        for kind, back in ways:
            direct_copy(m, kind, back, 0).wait_recv()
            onward_copy(m, kind, back).start()

    def spread(m):
        for kind, back in ways:
            direct_copy(m, kind, back, 1).wait_recv()
            onward_copy(m, kind, back).wait_recv()
        drain(turned[m].at[pl.ds(0, 14)], y_send.at[m])
        for d in HOPS + (0,):
            for kind in range(2):

                def one(k, carry):
                    code = table[kind * 2 + 1, d * 8 + k]
                    near = code % 128
                    hop = code // 16384 % 2
                    rank = code // 128 % 128
                    stay = code // 32768 > 0
                    for half in range(2):
                        here = middle[m][near + 16 * half]
                        there = landed[m][kind, hop, rank % 64 + rank // 64 * most, half]
                        brick = lax.select(jnp.broadcast_to(stay, here.shape), here, there)
                        if d == 0:
                            out[m, kind, (z, x)[kind], half, k] = brick
                        else:
                            turned[m][(kind * 3 + d - 1) * 2 + half, k] = brick
                    return carry

                lax.fori_loop(0, 8, one, 0)
                if d:
                    last_copy(m, kind, d).start()

    def settle(m):
        for kind in range(2):
            for d in HOPS:
                last_copy(m, kind, d).wait_recv()
        if m == MATS - 1:
            return

        def one(k, carry):
            def load(b):
                return out[m, (b // 4) % 2, b % 4, b // 8, k]

            def store(b, brick):
                out[m, (b // 4) % 2, b % 4, b // 8, k] = brick

            found[k] = quantize(load, store, columns)
            return carry

        lax.fori_loop(0, 8, one, 0)
        scales[m] = jnp.concatenate([found[k] for k in range(8)], axis=1)

    for m in range(MATS):
        start(m)
    turn(0, 0, 1)
    turn(1, 0, 1)
    turn(0, 1, 4)
    turn(1, 1, 4)
    turn(2, 0, 1)
    gather(0)
    turn(2, 1, 4)
    relay(0)
    gather(1)
    spread(0)
    relay(1)
    gather(2)
    spread(1)
    relay(2)
    settle(0)
    spread(2)
    settle(1)
    settle(2)

    for m in range(MATS):
        drain(first[m].at[pl.ds(1, 3)], first_send.at[m])
        for kind, back in ways:
            if m:
                for part in range(2):
                    direct_copy(m, kind, back, part).wait_send()
            onward_copy(m, kind, back).wait_send()
        drain(turned[m].at[pl.ds(0, 12)], last_send.at[m])


def write_kernel(moved, early, packed, scales, ready, found, early_sem, sem):
    columns = moved.shape[-2]
    last = MATS - 1

    def early_copy(m, k, b):
        return pltpu.make_async_copy(
            moved.at[m, (b // 4) % 2, b % 4, b // 8, k],
            packed.at[m, 0, 0, k, :, pl.ds(b * BLOCK, BLOCK)],
            early_sem.at[m],
        )

    def late_copy(k):
        return pltpu.make_async_copy(ready.at[k], packed.at[last, 0, 0, k], sem.at[k])

    for m in range(last):

        def issue(k, carry):
            for b in range(16):
                early_copy(m, k, b).start()
            return carry

        lax.fori_loop(0, 8, issue, 0)

    def one(k, carry):
        def load(b):
            return moved[last, (b // 4) % 2, b % 4, b // 8, k]

        def store(b, brick):
            ready[k, :, b * BLOCK : (b + 1) * BLOCK] = brick

        found[k] = quantize(load, store, columns)
        late_copy(k).start()
        return carry

    lax.fori_loop(0, 8, one, 0)
    for m in range(last):
        scales[m, 0, 0] = early[m]
    scales[last, 0, 0] = jnp.concatenate([found[k] for k in range(8)], axis=1)
    for m in range(last):
        drain(packed.at[m], early_sem.at[m])
    for k in range(8):
        late_copy(k).wait()


def move_kernel(index_ref, gate, up, down, out, *scratch):
    first = scratch[0:3]
    second = scratch[3:6]
    own = scratch[6]
    turned = scratch[7:10]
    middle = scratch[10:13]
    sorted_ = scratch[13:16]
    relay = scratch[16:19]
    own_sem, first_send, first_recv, second_send, second_recv = scratch[19:24]
    y_send, y_recv, third_send, third_recv, last_send, last_recv, keep_sem = scratch[24:31]
    weights = (gate, up, down)

    g = lax.axis_index("grp")
    q = lax.axis_index("sub")
    x, z, yl = g // 8, (g // 2) % 4, g % 2
    core = q % 2
    s8 = yl * 4 + q

    def device(xx, zz, ss):
        return ((xx * 4 + zz) * 2 + ss // 4, ss % 4)

    def pick(a, b):
        return jnp.where(core == 0, a, b)

    def flip(a, b):
        low = (a + b) % 2
        high = (a // 2 + b // 2) % 2
        return high * 2 + low

    x_to = [(x + d) % 4 for d in range(4)]
    z_to = [(z + d) % 4 for d in range(4)]
    x_from = [(x + 4 - d) % 4 for d in range(4)]
    z_from = [(z + 4 - d) % 4 for d in range(4)]
    dev1 = [device(pick(x, x_to[d]), pick(z_to[d], z), s8) for d in range(4)]
    dev2 = [device(pick(x_to[d], x), pick(z, z_to[d]), s8) for d in range(4)]
    s8_to = [(flip((s8 // 4) * 2 + (s8 // 2) % 2, r // 2)) * 2 + (s8 + r) % 2 for r in range(8)]
    dev_y = [device(x, z, s8_to[r]) for r in range(8)]

    barrier = pltpu.get_barrier_semaphore()
    partners = dev1[1:] + dev2[1:] + dev_y[1:]
    for partner in partners:
        pl.semaphore_signal(barrier, inc=1, device_id=partner, device_id_type=MESH)
    pl.semaphore_wait(barrier, len(partners))

    tile2 = [pick(flip(q, x_to[d]), z_to[d]) for d in range(4)]

    def source(m, d1, t):
        slot = pick(t, flip(q, x_to[d1]))
        block = pick(z_to[d1], t)
        return weights[m].at[slot, pl.ds(pl.multiple_of(block * BLOCK, BLOCK), BLOCK), :]

    def first_copy(m, d1, d2):
        t = tile2[d2]
        return pltpu.make_async_remote_copy(
            src_ref=source(m, d1, t),
            dst_ref=first[m].at[d1 - 1, t],
            send_sem=first_send.at[m],
            recv_sem=first_recv.at[m, d1 - 1, t],
            device_id=dev1[d1],
            device_id_type=MESH,
        )

    def second_copy(m, d1, d2):
        t = tile2[d2]
        return pltpu.make_async_remote_copy(
            src_ref=source(m, 0, t) if d1 == 0 else first[m].at[d1 - 1, t],
            dst_ref=second[m].at[d2 - 1, d1],
            send_sem=second_send.at[m],
            recv_sem=second_recv.at[m, d2 - 1, d1],
            device_id=dev2[d2],
            device_id_type=MESH,
        )

    def own_copy(m):
        return pltpu.make_async_copy(source(m, 0, tile2[0]), own.at[m], own_sem.at[m])

    def start_first(m):
        for d2 in (1, 3, 2, 0):
            for d1 in HOPS:
                first_copy(m, d1, d2).start()
        for d2 in HOPS:
            second_copy(m, 0, d2).start()
        own_copy(m).start()

    def forward(m):
        for d2 in (1, 3, 2, 0):
            for d1 in HOPS:
                first_copy(m, d1, d2).wait_recv()
                if d2:
                    second_copy(m, d1, d2).start()

    units, columns = turned[0].shape[1], turned[0].shape[2]

    def y_copy(m, r):
        return pltpu.make_async_remote_copy(
            src_ref=turned[m].at[:, s8_to[r]],
            dst_ref=middle[m].at[pl.ds(s8 * 16, 16)],
            send_sem=y_send.at[m],
            recv_sem=y_recv.at[m, r - 1],
            device_id=dev_y[r],
            device_id_type=MESH,
        )

    def place_of(d1, d2):
        x_back, z_back = pick(d2, d1), pick(d1, d2)
        return (x + 4 - x_back) % 4 * 4 + (z + 4 - z_back) % 4

    def turn_and_cross(m):
        own_copy(m).wait()

        def turn(tile, place):
            turned[m][place] = tile.T.reshape(units, columns, BLOCK)

        turn(own[m], place_of(0, 0))

        def near(i, carry):
            turn(first[m][i, tile2[0]], place_of(i + 1, 0))
            return carry

        lax.fori_loop(0, 3, near, 0)
        for d1 in (0,) + HOPS:
            for d2 in HOPS:
                second_copy(m, d1, d2).wait_recv()

        def far(i, carry):
            turn(second[m][i // 4, i % 4], place_of(i % 4, i // 4 + 1))
            return carry

        lax.fori_loop(0, 12, far, 0)
        for r in range(1, 8):
            y_copy(m, r).start()
        middle[m][pl.ds(s8 * 16, 16)] = turned[m][:, s8]

    def third_copy(m, d1, t):
        return pltpu.make_async_remote_copy(
            src_ref=sorted_[m].at[pick(t, x_to[d1]), pick(z_to[d1], t)],
            dst_ref=relay[m].at[d1 - 1, t],
            send_sem=third_send.at[m],
            recv_sem=third_recv.at[m, d1 - 1, t],
            device_id=dev1[d1],
            device_id_type=MESH,
        )

    def last_source(m, d1, d2):
        t = pick(x_to[d2], z_to[d2])
        if d1 == 0:
            return sorted_[m].at[pick(t, x), pick(z, t)]
        return relay[m].at[d1 - 1, t]

    def last_place(m, d1):
        return out.at[m, pick(x * 4 + z_from[d1], x_from[d1] * 4 + z)]

    def last_copy(m, d1, d2):
        return pltpu.make_async_remote_copy(
            src_ref=last_source(m, d1, d2),
            dst_ref=last_place(m, d1),
            send_sem=last_send.at[m],
            recv_sem=last_recv.at[m],
            device_id=dev2[d2],
            device_id_type=MESH,
        )

    def keep_copy(m, d1):
        return pltpu.make_async_copy(last_source(m, d1, 0), last_place(m, d1), keep_sem.at[m, d1])

    def third_tile(d2):
        return pick(x_to[d2], z_to[d2])

    def permute(m):
        for r in range(1, 8):
            y_copy(m, r).wait_recv()

        def step(t, carry):
            for k in range(8):
                sorted_[m][t // 4, t % 4, k] = middle[m][index_ref[t * 8 + k]]
            return carry

        lax.fori_loop(0, 16, step, 0)
        for d2 in (1, 3, 2, 0):
            for d1 in HOPS:
                third_copy(m, d1, third_tile(d2)).start()
        for d2 in HOPS:
            last_copy(m, 0, d2).start()
        keep_copy(m, 0).start()

    def finish(m):
        for d2 in (1, 3, 2, 0):
            for d1 in HOPS:
                third_copy(m, d1, third_tile(d2)).wait_recv()
                if d2:
                    last_copy(m, d1, d2).start()
                else:
                    keep_copy(m, d1).start()

    start_first(0)
    start_first(1)
    start_first(2)
    forward(0)
    forward(1)
    turn_and_cross(0)
    forward(2)
    turn_and_cross(1)
    permute(0)
    turn_and_cross(2)
    finish(0)
    permute(1)
    finish(1)
    permute(2)
    finish(2)

    def drain(ref, sem):
        pltpu.make_async_copy(ref, ref, sem).wait()

    for m in range(MATS):
        drain(first[m], first_send.at[m])
        drain(second[m], second_send.at[m])
        drain(middle[m].at[pl.ds(0, 112)], y_send.at[m])
        drain(relay[m], third_send.at[m])
        drain(relay[m], last_send.at[m])
        drain(relay[m], last_recv.at[m])
        for d1 in range(4):
            keep_copy(m, d1).wait()


def scale_kernel(low_ref, moved, packed, scales, ready, found, sem):
    columns = moved.shape[3]
    lane = lax.broadcasted_iota(jnp.int32, (columns, BLOCK), 1)

    def out_copy(m, k):
        return pltpu.make_async_copy(ready.at[m, k], packed.at[m, 0, 0, k], sem.at[m, k])

    for m in range(MATS):

        def step(k, carry):
            low = low_ref[k]
            seen = jnp.zeros((columns, BLOCK), jnp.float32)
            for b in range(16):
                place = ((b // 4) ^ low) * 4 + b % 4
                values = moved[m, place, k].astype(jnp.float32)
                scale = jnp.max(jnp.abs(values), axis=1, keepdims=True) + EPS
                ready[m, k, :, b * BLOCK : (b + 1) * BLOCK] = (values * (1.0 / scale)).astype(jnp.bfloat16)
                seen = jnp.where(lane == b, scale, seen)
            found[k] = seen.T[:16]
            out_copy(m, k).start()
            return carry

        lax.fori_loop(0, 8, step, 0)
        scales[m, 0, 0] = jnp.concatenate([found[k] for k in range(8)], axis=1)

    for m in range(MATS):
        for k in range(8):
            out_copy(m, k).wait()


def through(table, gate, up, down, source_order, target_order):
    slots, rows, hidden = gate.shape
    columns = hidden // 8
    experts = source_order.shape[0]
    matches = (source_order[None, :] == target_order[:, None]).astype(jnp.int32)
    picked = jnp.sum(matches * jnp.arange(experts, dtype=jnp.int32)[None, :], axis=1)
    g = lax.axis_index("grp")
    x = g // 8
    col, yl, low = picked // 8, (picked // 4) % 2, picked % 4
    index = (yl * 4 + (low ^ x)) * 16 + col

    tile = (BLOCK, hidden)
    brick = (columns, BLOCK)
    bf16 = jnp.bfloat16
    dma = pltpu.SemaphoreType.DMA
    any_space = pl.BlockSpec(memory_space=pl.ANY)
    scratch = (
        [pltpu.VMEM((3, 4) + tile, bf16)] * 3
        + [pltpu.VMEM((3, 4) + tile, bf16)] * 3
        + [pltpu.VMEM((3,) + tile, bf16)]
        + [pltpu.VMEM((16, 8) + brick, bf16)] * 3
        + [pltpu.VMEM((128,) + brick, bf16)] * 3
        + [pltpu.VMEM((4, 4, 8) + brick, bf16)] * 3
        + [pltpu.VMEM((3, 4, 8) + brick, bf16)] * 3
        + [dma((3,)), dma((3,)), dma((3, 3, 4)), dma((3,)), dma((3, 3, 4))]
        + [dma((3,)), dma((3, 7)), dma((3,)), dma((3, 3, 4)), dma((3,)), dma((3,)), dma((3, 4))]
    )
    moved = pl.pallas_call(
        move_kernel,
        out_shape=pltpu.VMEM((3, 16, 8) + brick, bf16),
        in_specs=[pl.BlockSpec(memory_space=pltpu.SMEM), any_space, any_space, any_space],
        out_specs=pl.BlockSpec(memory_space=pltpu.VMEM),
        scratch_shapes=scratch,
        compiler_params=pltpu.CompilerParams(
            collective_id=2, has_side_effects=True, vmem_limit_bytes=51 * 2**20
        ),
        name="move",
    )(index, gate, up, down)

    mine = lax.dynamic_slice(low, ((g // 2) * 8,), (8,))
    return pl.pallas_call(
        scale_kernel,
        in_specs=[pl.BlockSpec(memory_space=pltpu.SMEM), pl.BlockSpec(memory_space=pltpu.VMEM)],
        out_specs=[any_space, pl.BlockSpec(memory_space=pltpu.VMEM)],
        out_shape=[
            jax.ShapeDtypeStruct((3, 1, 1, 8, columns, 16 * BLOCK), bf16),
            jax.ShapeDtypeStruct((3, 1, 1, 16, hidden), jnp.float32),
        ],
        scratch_shapes=[pltpu.VMEM((3, 8, columns, 16 * BLOCK), bf16), pltpu.VMEM((8, 16, columns), jnp.float32), dma((3, 8))],
        compiler_params=pltpu.CompilerParams(vmem_limit_bytes=20 * 2**20),
        name="scale",
    )(mine, moved)


def per_device(gate, up, down, source_order, target_order):
    slots, rows, hidden = gate.shape
    columns = hidden // 8
    tile = (BLOCK, hidden)
    brick = (columns, BLOCK)
    bf16, f32 = jnp.bfloat16, jnp.float32
    dma = pltpu.SemaphoreType.DMA
    any_space = pl.BlockSpec(memory_space=pl.ANY)
    smem = pl.BlockSpec(memory_space=pltpu.SMEM)
    vmem = pl.BlockSpec(memory_space=pltpu.VMEM)
    results = [
        jax.ShapeDtypeStruct((3, 1, 1, 8, columns, 16 * BLOCK), bf16),
        jax.ShapeDtypeStruct((3, 1, 1, 16, hidden), f32),
    ]

    table, level = pl.pallas_call(
        plan_kernel,
        out_shape=[
            jax.ShapeDtypeStruct((8, 128), jnp.int32),
            jax.ShapeDtypeStruct((1,), jnp.int32),
        ],
        in_specs=[vmem, vmem],
        out_specs=[vmem, smem],
        name="plan",
    )(source_order[None, :], target_order[None, :])

    def direct(room, number, table, gate, up, down, source_order, target_order):
        scratch = (
            [pltpu.VMEM((4, 4) + tile, bf16)] * 3
            + [pltpu.VMEM((16, 8) + brick, bf16)] * 3
            + [pltpu.VMEM((128,) + brick, bf16)] * 3
            + [pltpu.VMEM((2, 2, room[0], 2) + brick, bf16)] * 2
            + [pltpu.VMEM((2, 2, room[0] + room[1], 2) + brick, bf16)] * 3
            + [pltpu.VMEM((8, 16, columns), f32)]
            + [dma((3,)), dma((3, 4)), dma((3,)), dma((3, 7))]
            + [dma((3, 2, 2, 2))] * 2
            + [dma((3, 2, 2))] * 2
            + [dma((3,)), dma((3, 2, 3))]
        )
        moved, early = pl.pallas_call(
            functools.partial(direct_kernel, room),
            out_shape=[pltpu.VMEM((3, 2, 4, 2, 8) + brick, bf16), pltpu.VMEM((2, 16, hidden), f32)],
            in_specs=[smem, any_space, any_space, any_space],
            out_specs=[vmem, vmem],
            scratch_shapes=scratch,
            compiler_params=pltpu.CompilerParams(
                collective_id=number, has_side_effects=True, vmem_limit_bytes=50 * 2**20
            ),
            name="direct",
        )(table, gate, up, down)
        return pl.pallas_call(
            write_kernel,
            in_specs=[vmem, vmem],
            out_specs=[any_space, vmem],
            out_shape=results,
            scratch_shapes=[
                pltpu.VMEM((8, columns, 16 * BLOCK), bf16),
                pltpu.VMEM((8, 16, columns), f32),
                dma((2,)),
                dma((8,)),
            ],
            compiler_params=pltpu.CompilerParams(vmem_limit_bytes=12 * 2**20),
            name="write",
        )(moved, early)

    operands = (table, gate, up, down, source_order, target_order)
    ways = [functools.partial(direct, room, 3 + i) for i, room in enumerate(ROOMS)]
    return tuple(lax.switch(level[0], ways + [through], *operands))


def solution(mesh):
    placed = (P("grp", "sub", None), P("grp", "sub", None), P("grp", "sub", None), P(), P())
    return jax.shard_map(
        per_device,
        mesh=mesh,
        in_specs=placed,
        out_specs=(P(None, "grp", "sub", None, None, None), P(None, "grp", "sub", None, None)),
        check_vma=False,
    )
```
